256 devices in a mesh: tok: 32 (over z, x), reg: 8 (over y, core).
Axes of the slice: x: 4, y: 4, z: 8, core: 2. Of those that a mesh axis runs over, the one named last changes fastest.
Arguments:
- tokens: bfloat16 [65536, 1024], P(('reg', 'tok')), parts along dimension 0, may hold values from -256 to 256
- valid_count: int32 [8], P('reg'), parts along dimension 0, may hold values from 4096 to 8192
- latents: bfloat16 [512, 1024], replicated, may hold values from -256 to 256
- key_weight: bfloat16 [1024, 1024], replicated, may hold values from -0.4375 to 0.4375
- value_weight: bfloat16 [1024, 1024], replicated, may hold values from -0.375 to 0.375
- query_weight: bfloat16 [1024, 1024], replicated, may hold values from -0.1875 to 0.1875
- latent_key_weight: bfloat16 [1024, 1024], replicated, may hold values from -0.375 to 0.375
- latent_value_weight: bfloat16 [1024, 1024], replicated, may hold values from -0.375 to 0.375
Outputs:
- decoded: bfloat16 [65536, 1024], P(('reg', 'tok')), parts along dimension 0
The draws below stay inside these ranges and needn't reach their ends.
There are 8 independent parts, one for each index of `reg`. The reference program is written for one: setup_inputs(seed, part) draws one part's arguments, and reference() takes and returns one part's arrays. A program takes and returns all parts, laid end to end along the dimension named above; an argument that names none is the same for every part. Nothing has to cross between parts.
Inputs may be any that keep to these rules, and one draw needn't show every extreme that they name: The valid tokens are the first valid_count[0] of the region.
All inputs are finite; a program needn't handle non-finite values.
Results may differ from the reference program's by a relative error of at most 0.01.
The reference program's roundings to bfloat16 on the way count: a program that leaves them out, or rounds other values in their place, can miss the bound.
Values may be sent and summed in bfloat16 or wider, within the bound.
No kernel may reach another device: no remote copies, remote signals or barrier semaphores. Data moves between devices by JAX's collectives and lax.ppermute only.
A program may use at most 64 MiB of HBM per device.

```python
import jax
import jax.numpy as jnp
from jax import lax

D = 1024
LATENTS = 512
HEADS = 16
HEAD_DIM = 64
TOKENS = 8192


def scaled_rows(key, row_count, width):
    first = jax.random.fold_in(key, 0)
    base = jnp.clip(jax.random.normal(first, (row_count, width), jnp.float32), -4.0, 4.0)
    return base


def draw_tokens(key, part):
    return scaled_rows(jax.random.fold_in(key, 11), TOKENS, D).astype(jnp.bfloat16)


def draw_latents(key, part):
    return scaled_rows(jax.random.fold_in(key, 23), LATENTS, D).astype(jnp.bfloat16)


def bell_draw(rng, extent, deviation, reach, held_as=jnp.bfloat16):
    values = deviation * jax.random.normal(rng, extent, jnp.float32)
    return jnp.clip(values, min=-reach, max=reach).astype(held_as)


def setup_inputs(seed: int = 0, part: int = 0) -> dict:
    streams_of = jax.random.split(jax.random.key(seed), 9)
    own_keys = jax.random.split(jax.random.fold_in(streams_of[8], part), 9)
    tokens = draw_tokens(jax.random.fold_in(jax.random.fold_in(streams_of[8], part), 71), part)
    valid_count = jax.random.randint(own_keys[1], (1,), TOKENS // 2, TOKENS + 1).astype(jnp.int32)
    latents = draw_latents(jax.random.fold_in(streams_of[8], 71), part)
    key_weight = bell_draw(streams_of[3], (D, D), (D // 6) ** -0.5, 0.4375)
    value_weight = bell_draw(streams_of[4], (D, D), (D // 4) ** -0.5, 0.375)
    query_weight = bell_draw(streams_of[5], (D, D), D ** -0.5, 0.1875)
    latent_key_weight = bell_draw(streams_of[6], (D, D), (D // 4) ** -0.5, 0.375)
    latent_value_weight = bell_draw(streams_of[7], (D, D), (D // 4) ** -0.5, 0.375)
    return {"tokens": tokens, "valid_count": valid_count, "latents": latents, "key_weight": key_weight, "value_weight": value_weight, "query_weight": query_weight, "latent_key_weight": latent_key_weight, "latent_value_weight": latent_value_weight}


def heads_first(array):
    return array.reshape(array.shape[0], HEADS, HEAD_DIM).transpose(1, 0, 2).astype(jnp.float32)

def reference(tokens, valid_count, latents, key_weight, value_weight, query_weight, latent_key_weight, latent_value_weight):
    score_scale = 1.0 / HEAD_DIM ** 0.5
    keys = jnp.dot(tokens, key_weight, preferred_element_type=jnp.float32).astype(jnp.bfloat16)
    values = jnp.dot(tokens, value_weight, preferred_element_type=jnp.float32).astype(jnp.bfloat16)
    position = jnp.arange(TOKENS, dtype=jnp.int32)
    valid = position < valid_count[0]

    def encode_head(operands):
        query, key_head, value_head = operands
        scores = jnp.dot(query, key_head.T, preferred_element_type=jnp.float32) * score_scale
        scores = jnp.where(valid[None, :], scores, -1e+30)
        top = lax.optimization_barrier(jnp.max(scores, axis=1, keepdims=True))
        weights = jnp.where(valid[None, :], jnp.exp(scores - top), 0.0)
        total = lax.optimization_barrier(jnp.sum(weights, axis=1, keepdims=True))
        summed = jnp.dot(weights.astype(jnp.bfloat16).astype(jnp.float32), value_head, preferred_element_type=jnp.float32)
        return summed / total
    attended = lax.map(encode_head, (heads_first(latents), heads_first(keys), heads_first(values)))
    attended = attended.transpose(1, 0, 2).reshape(LATENTS, D)
    encoded = latents.astype(jnp.float32) + attended
    normed = (encoded * lax.rsqrt(lax.optimization_barrier(jnp.mean(encoded * encoded, axis=1, keepdims=True)) + 1e-06)).astype(jnp.bfloat16)
    latent_keys = jnp.dot(normed, latent_key_weight, preferred_element_type=jnp.float32).astype(jnp.bfloat16)
    latent_values = jnp.dot(normed, latent_value_weight, preferred_element_type=jnp.float32).astype(jnp.bfloat16)
    queries = jnp.dot(tokens, query_weight, preferred_element_type=jnp.float32).astype(jnp.bfloat16)

    def decode_head(operands):
        query, key_head, value_head = operands
        scores = jnp.dot(query, key_head.T, preferred_element_type=jnp.float32) * score_scale
        top = lax.optimization_barrier(jnp.max(scores, axis=1, keepdims=True))
        weights = jnp.exp(scores - top)
        total = lax.optimization_barrier(jnp.sum(weights, axis=1, keepdims=True))
        summed = jnp.dot(weights.astype(jnp.bfloat16).astype(jnp.float32), value_head, preferred_element_type=jnp.float32)
        return summed / total
    decoded_heads = lax.map(decode_head, (heads_first(queries), heads_first(latent_keys), heads_first(latent_values)))
    decoded_heads = decoded_heads.transpose(1, 0, 2).reshape(TOKENS, D)
    return (tokens.astype(jnp.float32) + decoded_heads).astype(jnp.bfloat16)
```

```python
import functools
import math

import jax
import jax.numpy as jnp
from jax import lax
from jax.experimental import pallas as pl
from jax.experimental.pallas import tpu as pltpu
from jax.sharding import Mesh, PartitionSpec as P

D = 1024
HEADS = 16
LATENTS = 512
ROWS = 256
NX = 4
NZ = 8
GROUP = D // NX
SCALE = 0.125
EXP2_SCALE = SCALE * math.log2(math.e)
VMEM_BYTES = 24 * 1024 * 1024


F32 = jnp.float32
BF16 = jnp.bfloat16


def dot(a, b):
    return jnp.dot(a, b, preferred_element_type=F32)


def dot_t(a, b):
    return lax.dot_general(a, b, (((1,), (1,)), ((), ())), preferred_element_type=F32)


def lane_half(shape):
    return lax.broadcasted_iota(jnp.int32, shape, 1) < 64


def kv_body(where, tok, wk, wv, out):
    t = tok[...]
    out[:, :GROUP] = dot(t, wk[...]).astype(BF16)
    out[:, GROUP:] = dot(t, wv[...]).astype(BF16)


def kv_for(offset, where, tokens, key_weight, value_weight):
    def columns(i, where):
        return (0, lax.rem(where[0] + offset, NX))

    return pl.pallas_call(
        kv_body,
        out_shape=jax.ShapeDtypeStruct((ROWS, 2 * GROUP), BF16),
        grid_spec=pltpu.PrefetchScalarGridSpec(
            num_scalar_prefetch=1,
            grid=(1,),
            in_specs=[
                pl.BlockSpec((ROWS, D), lambda i, w: (0, 0)),
                pl.BlockSpec((D, GROUP), columns),
                pl.BlockSpec((D, GROUP), columns),
            ],
            out_specs=pl.BlockSpec((ROWS, 2 * GROUP), lambda i, w: (0, 0)),
        ),
        compiler_params=pltpu.CompilerParams(vmem_limit_bytes=VMEM_BYTES),
        cost_estimate=pl.CostEstimate(
            flops=4 * ROWS * D * GROUP, bytes_accessed=2 * D * GROUP * 2 + ROWS * D * 3, transcendentals=0
        ),
        name="kv_proj",
    )(where, tokens, key_weight, value_weight)


def attend_body(where, lat, kv0, kv1, kv2, kv3, out):
    x, z, count = where[0], where[1], where[2]
    chunks = (kv0, kv1, kv2, kv3)
    lane = lax.broadcasted_iota(jnp.int32, (1, ROWS), 1)
    valid = [
        (z * NX + lax.rem(x + (NX - c), NX)) * ROWS + lane < count for c in range(NX)
    ]
    block = 256
    for b in range(LATENTS // block):
        rows = slice(b * block, (b + 1) * block)
        stat_lane = lax.broadcasted_iota(jnp.int32, (block, 128), 1)
        stat_row = lax.broadcasted_iota(jnp.int32, (block, 128), 0)
        place = stat_lane - ((stat_row >> 4) & 3) * 4
        stats = jnp.zeros((block, 128), F32)
        means = []
        for p in range(2):
            lat_pair = lat[rows, p * 128 : (p + 1) * 128]
            halves = []
            for hh in range(2):
                left = lane_half((block, 128))
                keep = left if hh == 0 else jnp.logical_not(left)
                query = jnp.where(keep, lat_pair, jnp.zeros_like(lat_pair))
                scores = [
                    jnp.where(valid[c], dot_t(query, chunks[c][:, p * 128 : (p + 1) * 128]), -1e30)
                    for c in range(NX)
                ]
                top = jnp.maximum(
                    jnp.maximum(scores[0], scores[1]), jnp.maximum(scores[2], scores[3])
                )
                peak = jnp.maximum(jnp.max(top, axis=1, keepdims=True), -1e29)
                weights = [jnp.exp2((s - peak) * EXP2_SCALE) for s in scores]
                total = jnp.sum(
                    (weights[0] + weights[1]) + (weights[2] + weights[3]), axis=1, keepdims=True
                )
                total = jnp.maximum(total, 1.0)
                summed = sum(
                    dot(weights[c].astype(BF16), chunks[c][:, GROUP + p * 128 : GROUP + (p + 1) * 128])
                    for c in range(NX)
                )
                halves.append(summed / total)
                lse = peak * SCALE + jnp.log(total)
                h = 2 * p + hh
                rest = lse
                for piece in range(3):
                    part = rest.astype(BF16).astype(F32)
                    rest = rest - part
                    stats = jnp.where(place == piece * 16 + h, part, stats)
            means.append(jnp.where(lane_half((block, 128)), halves[0], halves[1]).astype(BF16))
        for d in range(block // 64):
            dest = b * (block // 64) + d
            for g in range(4):
                r = slice(d * 64 + g * 16, d * 64 + (g + 1) * 16)
                for p in range(2):
                    out[dest, :, g * GROUP + p * 128 : g * GROUP + (p + 1) * 128] = means[p][r, :]
            keep = stats[d * 64 : d * 64 + 16]
            for g in range(1, 4):
                keep = keep + stats[d * 64 + g * 16 : d * 64 + (g + 1) * 16]
            out[dest, :, D : D + 128] = keep.astype(BF16)


def attend(where, latents, kvs):
    return pl.pallas_call(
        attend_body,
        out_shape=jax.ShapeDtypeStruct((NZ, 16, D + 128), BF16),
        grid_spec=pltpu.PrefetchScalarGridSpec(
            num_scalar_prefetch=1,
            grid=(1,),
            in_specs=[pl.BlockSpec((LATENTS, GROUP), lambda i, w: (0, w[0]))]
            + [pl.BlockSpec((ROWS, 2 * GROUP), lambda i, w: (0, 0))] * NX,
            out_specs=pl.BlockSpec((NZ, 16, D + 128), lambda i, w: (0, 0, 0)),
        ),
        compiler_params=pltpu.CompilerParams(vmem_limit_bytes=VMEM_BYTES),
        cost_estimate=pl.CostEstimate(
            flops=4 * LATENTS * ROWS * NX * GROUP,
            bytes_accessed=2 * 1024 * 1024,
            transcendentals=LATENTS * ROWS * NX * 4,
        ),
        name="attend",
    )(where, latents, *kvs)


def merge_body(parts, out):
    stats = parts[:, :, D : D + 128].reshape(NZ * 16, 128)
    j = lax.broadcasted_iota(jnp.int32, (128, D), 0)
    n = lax.broadcasted_iota(jnp.int32, (128, D), 1)
    spread = jnp.where(((j & 15) == (n >> 6)) & (j < 48), 1.0, 0.0).astype(BF16)
    lse = dot(stats, spread).reshape(NZ, 16, D)
    peak = jnp.max(lse, axis=0)
    num = jnp.zeros((16, D), F32)
    den = jnp.zeros((16, D), F32)
    for s in range(NZ):
        w = jnp.exp(lse[s] - peak)
        den = den + w
        num = num + w * parts[s, :, :D].astype(F32)
    att = (num / den).astype(BF16)
    for g in range(4):
        for d in range(NZ):
            out[d, g * 16 : (g + 1) * 16, :] = att[:, g * GROUP : (g + 1) * GROUP]


def merge(parts):
    return pl.pallas_call(
        merge_body,
        out_shape=jax.ShapeDtypeStruct((NZ, 64, GROUP), BF16),
        compiler_params=pltpu.CompilerParams(vmem_limit_bytes=VMEM_BYTES),
        cost_estimate=pl.CostEstimate(
            flops=2 * 128 * 128 * D, bytes_accessed=1024 * 1024, transcendentals=128 * D
        ),
        name="merge",
    )(parts)


def query_body(tok, wq, out):
    out[...] = dot(tok[...], wq[...]).astype(BF16)


def project_queries(tokens, query_weight):
    return pl.pallas_call(
        query_body,
        out_shape=jax.ShapeDtypeStruct((ROWS, D), BF16),
        compiler_params=pltpu.CompilerParams(vmem_limit_bytes=VMEM_BYTES),
        cost_estimate=pl.CostEstimate(
            flops=2 * ROWS * D * D, bytes_accessed=3 * 1024 * 1024, transcendentals=0
        ),
        name="q_proj",
    )(tokens, query_weight)


def decode_body(where, lat, a0, a1, a2, a3, wk, wv, q, tok, out, enc, lk, lv):
    x = where[0]
    square = jnp.zeros((LATENTS, 1), F32)
    for c, a in enumerate((a0, a1, a2, a3)):
        start = pl.multiple_of(lax.rem(x + (NX - c), NX) * GROUP, GROUP)
        e = lat[:, pl.ds(start, GROUP)].astype(F32) + a[...].astype(F32)
        square = square + jnp.sum(e * e, axis=1, keepdims=True)
        enc[:, pl.ds(start, GROUP)] = e
    scale = lax.rsqrt(square * (1.0 / D) + 1e-06)
    normed = (enc[...] * scale).astype(BF16)
    lk[...] = dot(normed, wk[...]).astype(BF16)
    lv[...] = dot(normed, wv[...]).astype(BF16)
    left = lane_half((ROWS, 128))
    for p in range(HEADS // 2):
        cols = slice(p * 128, (p + 1) * 128)
        q_pair = q[:, cols]
        halves = []
        for hh in range(2):
            keep = left if hh == 0 else jnp.logical_not(left)
            query = jnp.where(keep, q_pair, jnp.zeros_like(q_pair))
            scores = dot_t(query, lk[:, cols])
            peak = jnp.max(scores, axis=1, keepdims=True)
            weights = jnp.exp2((scores - peak) * EXP2_SCALE)
            total = jnp.sum(weights, axis=1, keepdims=True)
            halves.append(dot(weights.astype(BF16), lv[:, cols]) / total)
        both = jnp.where(left, halves[0], halves[1])
        out[:, cols] = (tok[:, cols].astype(F32) + both).astype(BF16)


def decode(where, latents, attended, wk, wv, queries, tokens):
    full = lambda *shape: pl.BlockSpec(shape, lambda i, w: (0,) * len(shape))
    return pl.pallas_call(
        decode_body,
        out_shape=jax.ShapeDtypeStruct((ROWS, D), BF16),
        grid_spec=pltpu.PrefetchScalarGridSpec(
            num_scalar_prefetch=1,
            grid=(1,),
            in_specs=[full(LATENTS, D)]
            + [full(LATENTS, GROUP)] * NX
            + [full(D, D), full(D, D), full(ROWS, D), full(ROWS, D)],
            out_specs=full(ROWS, D),
            scratch_shapes=[
                pltpu.VMEM((LATENTS, D), F32),
                pltpu.VMEM((LATENTS, D), BF16),
                pltpu.VMEM((LATENTS, D), BF16),
            ],
        ),
        compiler_params=pltpu.CompilerParams(vmem_limit_bytes=36 * 1024 * 1024),
        cost_estimate=pl.CostEstimate(
            flops=4 * LATENTS * D * D + 4 * ROWS * LATENTS * D,
            bytes_accessed=8 * 1024 * 1024,
            transcendentals=ROWS * LATENTS * HEADS,
        ),
        name="decode",
    )(where, latents, *attended, wk, wv, queries, tokens)


def shifted(value, offset):
    return lax.ppermute(value, "x", [(i, (i + offset) % NX) for i in range(NX)])


def per_device(
    tokens,
    valid_count,
    latents,
    key_weight,
    value_weight,
    query_weight,
    latent_key_weight,
    latent_value_weight,
):
    where = jnp.stack([lax.axis_index("x"), lax.axis_index("z"), valid_count[0]]).astype(jnp.int32)
    kvs = [None] * NX
    for offset in (2, 1, 3, 0):
        kv = kv_for(offset, where, tokens, key_weight, value_weight)
        kvs[offset] = shifted(kv, offset) if offset else kv
    queries = project_queries(tokens, query_weight)
    partial = attend(where, latents, kvs)
    parts = lax.all_to_all(partial, "z", 0, 0, tiled=True)
    merged = merge(parts)
    rows = lax.all_to_all(merged, "z", 0, 0, tiled=True).reshape(LATENTS, GROUP)
    attended = [rows] + [shifted(rows, offset) for offset in (1, 2, 3)]
    return decode(where, latents, attended, latent_key_weight, latent_value_weight, queries, tokens)


def solution(mesh):
    split = Mesh(mesh.devices.reshape(NZ, NX, -1), ("z", "x", "reg"))
    spread = P(("reg", "z", "x"), None)
    placed = (spread, P("reg"), P(), P(), P(), P(), P(), P())
    return jax.shard_map(
        per_device, mesh=split, in_specs=placed, out_specs=spread, check_vma=False
    )
```

```python
import functools
import math

import jax
import jax.numpy as jnp
from jax import lax
from jax.experimental import pallas as pl
from jax.experimental.pallas import tpu as pltpu
from jax.sharding import Mesh, PartitionSpec as P

D = 1024
HEADS = 16
LATENTS = 512
ROWS = 256
NX = 4
NZ = 8
PEERS = 8
PAIR = 128
SCALE = 0.125
EXP2_SCALE = SCALE * math.log2(math.e)
MIB = 1024 * 1024


F32 = jnp.float32
BF16 = jnp.bfloat16
AXES = ("zh", "zl", "xh", "xl")
IN_VMEM = pl.BlockSpec(memory_space=pltpu.VMEM)
IN_HBM = pl.BlockSpec(memory_space=pltpu.HBM)
IN_SMEM = pl.BlockSpec(memory_space=pltpu.SMEM)


def dot(a, b):
    return jnp.dot(a, b, preferred_element_type=F32)


def dot_t(a, b):
    return lax.dot_general(a, b, (((1,), (1,)), ((), ())), preferred_element_type=F32)


def left_half(shape):
    return lax.broadcasted_iota(jnp.int32, shape, 1) < 64


def both_heads(pair):
    left = left_half(pair.shape)
    zero = jnp.zeros_like(pair)
    return jnp.concatenate([jnp.where(left, pair, zero), jnp.where(left, zero, pair)], axis=0)


def my_role():
    return lax.axis_index("zl") * 2 + lax.axis_index("xl")


def square_peer(z, x, k, tiling):
    if tiling == 0:
        return z ^ (k >> 1), x ^ (k & 1)
    dz = (2 * (z & 1) - 1) * (k >> 1)
    dx = (2 * (x & 1) - 1) * (k & 1)
    return (z + dz) & (NZ - 1), (x + dx) & (NX - 1)


def send(value, k, tiling):
    pairs = []
    for z in range(NZ):
        for x in range(NX):
            pz, px = square_peer(z, x, k, tiling)
            pairs.append((z * NX + x, pz * NX + px))
    return lax.ppermute(value, AXES, pairs)


KV_ORDER = (3, 1, 2, 0)


def kv_body(tok_hbm, wk_hbm, wv_hbm, *refs):
    outs, (tok, w, tok_sem, w_sem) = refs[:8], refs[8:]
    role = my_role()
    tok_copy = pltpu.make_async_copy(tok_hbm, tok, tok_sem)
    copies = []
    for n, k in enumerate(KV_ORDER):
        start = pl.multiple_of((role ^ k) * PAIR, PAIR)
        for t in range(2):
            for j, hbm in enumerate((wk_hbm, wv_hbm)):
                s = 2 * t + j
                copies.append(
                    pltpu.make_async_copy(
                        hbm.at[:, pl.ds(t * 512 + start, PAIR)],
                        w.at[n, :, pl.ds(s * PAIR, PAIR)],
                        w_sem.at[n, s],
                    )
                )
    tok_copy.start()
    for c in copies:
        c.start()
    tok_copy.wait()
    for n, k in enumerate(KV_ORDER):
        for c in copies[4 * n : 4 * n + 4]:
            c.wait()
        kv = dot(tok[...], w[n]).astype(BF16)
        outs[k][...] = kv[:, : 2 * PAIR]
        outs[4 + k][...] = kv[:, 2 * PAIR :]


def project_kv(tokens, key_weight, value_weight):
    return pl.pallas_call(
        kv_body,
        out_shape=[jax.ShapeDtypeStruct((ROWS, 2 * PAIR), BF16)] * 8,
        in_specs=[IN_HBM] * 3,
        out_specs=[IN_VMEM] * 8,
        scratch_shapes=[
            pltpu.VMEM((ROWS, D), BF16),
            pltpu.VMEM((4, D, 4 * PAIR), BF16),
            pltpu.SemaphoreType.DMA(()),
            pltpu.SemaphoreType.DMA((4, 4)),
        ],
        compiler_params=pltpu.CompilerParams(vmem_limit_bytes=64000 * 1024),
        cost_estimate=pl.CostEstimate(
            flops=4 * ROWS * D * D, bytes_accessed=6 * MIB, transcendentals=0
        ),
        name="kv_proj",
    )(tokens, key_weight, value_weight)


def prepare_body(tok, lat, wq, wk, wv, q, pk, pv):
    q[...] = dot(tok[...], wq[...]).astype(BF16)
    pk[...] = dot(lat[...], wk[...])
    pv[...] = dot(lat[...], wv[...])


def prepare(tokens, latents, wq, wk, wv):
    return pl.pallas_call(
        prepare_body,
        out_shape=[
            jax.ShapeDtypeStruct((ROWS, D), BF16),
            jax.ShapeDtypeStruct((LATENTS, D), F32),
            jax.ShapeDtypeStruct((LATENTS, D), F32),
        ],
        in_specs=[IN_VMEM] * 5,
        out_specs=[IN_VMEM] * 3,
        compiler_params=pltpu.CompilerParams(vmem_limit_bytes=20 * MIB),
        cost_estimate=pl.CostEstimate(
            flops=2 * ROWS * D * D + 4 * LATENTS * D * D, bytes_accessed=12 * MIB, transcendentals=0
        ),
        name="prepare",
    )(tokens, latents, wq, wk, wv)


def attend_body(tiling, count, lat, kv0, kv1, kv2, kv3, *refs):
    if tiling == 0:
        out, stat_out = refs
    else:
        first, first_stats, out = refs
    z = lax.axis_index("zh") * 2 + lax.axis_index("zl")
    x = lax.axis_index("xh") * 2 + lax.axis_index("xl")
    chunks = (kv0, kv1, kv2, kv3)
    lane = lax.broadcasted_iota(jnp.int32, (1, ROWS), 1)
    valid = []
    for k in range(4):
        pz, px = square_peer(z, x, k, tiling)
        valid.append((pz * NX + px) * ROWS + lane < count[0])
    start = pl.multiple_of(my_role() * PAIR, PAIR) + tiling * 512
    block = 256
    for b in range(LATENTS // block):
        rows = slice(b * block, (b + 1) * block)
        query = both_heads(lat[rows, pl.ds(start, PAIR)])
        scores = [jnp.where(valid[k], dot_t(query, chunks[k][:, :PAIR]), -1e30) for k in range(4)]
        top = jnp.maximum(jnp.maximum(scores[0], scores[1]), jnp.maximum(scores[2], scores[3]))
        peak = jnp.maximum(jnp.max(top, axis=1, keepdims=True), -1e29)
        weights = [jnp.exp2((s - peak) * EXP2_SCALE) for s in scores]
        total = jnp.sum((weights[0] + weights[1]) + (weights[2] + weights[3]), axis=1, keepdims=True)
        total = jnp.maximum(total, 1.0)
        summed = sum(dot(weights[k].astype(BF16), chunks[k][:, PAIR:]) for k in range(4))
        lse = peak * SCALE + jnp.log(total)
        left = left_half((block, PAIR))
        means = jnp.where(left, summed[:block], summed[block:]) / jnp.where(
            left, total[:block], total[block:]
        )
        means = means.astype(BF16)
        stat_lane = lax.broadcasted_iota(jnp.int32, (block, 128), 1)
        stat_row = lax.broadcasted_iota(jnp.int32, (block, 128), 0)
        place = stat_lane - ((stat_row >> 4) & 3) * 4
        stats = jnp.zeros((block, 128), F32) if tiling == 0 else first_stats[rows, :]
        for hh in range(2):
            rest = lse[hh * block : (hh + 1) * block]
            for piece in range(3):
                part = rest.astype(BF16).astype(F32)
                rest = rest - part
                stats = jnp.where(place == piece * 16 + 2 * tiling + hh, part, stats)
        if tiling == 0:
            stat_out[rows, :] = stats
        for d in range(block // 64):
            dest = b * (block // 64) + d
            for g in range(4):
                part = means[d * 64 + g * 16 : d * 64 + (g + 1) * 16, :]
                if tiling == 0:
                    out[dest, :, g * PAIR : (g + 1) * PAIR] = part
                else:
                    out[dest, :, 512 + g * PAIR : 512 + (g + 1) * PAIR] = part
            if tiling == 1:
                out[dest, :, :512] = first[dest]
                keep = stats[d * 64 : d * 64 + 16]
                for g in range(1, 4):
                    keep = keep + stats[d * 64 + g * 16 : d * 64 + (g + 1) * 16]
                out[dest, :, D : D + 128] = keep.astype(BF16)


def attend(tiling, count, latents, kvs, first=()):
    if tiling == 0:
        out_shape = [
            jax.ShapeDtypeStruct((PEERS, 16, 512), BF16),
            jax.ShapeDtypeStruct((LATENTS, 128), F32),
        ]
    else:
        out_shape = [jax.ShapeDtypeStruct((PEERS, 16, D + 128), BF16)]
    return pl.pallas_call(
        functools.partial(attend_body, tiling),
        out_shape=out_shape,
        in_specs=[IN_SMEM] + [IN_VMEM] * (5 + len(first)),
        out_specs=[IN_VMEM] * len(out_shape),
        compiler_params=pltpu.CompilerParams(vmem_limit_bytes=24 * MIB),
        cost_estimate=pl.CostEstimate(
            flops=4 * LATENTS * ROWS * 4 * PAIR,
            bytes_accessed=1 * MIB,
            transcendentals=LATENTS * ROWS * 8,
        ),
        name="attend",
    )(count, latents, *kvs, *first)


def merge_body(parts, out):
    stats = parts[:, :, D : D + 128].reshape(PEERS * 16, 128)
    j = lax.broadcasted_iota(jnp.int32, (128, D), 0)
    n = lax.broadcasted_iota(jnp.int32, (128, D), 1)
    head = ((n >> 7) & 3) * 4 + (n >> 9) * 2 + ((n >> 6) & 1)
    spread = jnp.where(((j & 15) == head) & (j < 48), 1.0, 0.0).astype(BF16)
    lse = dot(stats, spread).reshape(PEERS, 16, D)
    peak = jnp.max(lse, axis=0)
    num = jnp.zeros((16, D), F32)
    den = jnp.zeros((16, D), F32)
    for s in range(PEERS):
        w = jnp.exp(lse[s] - peak)
        den = den + w
        num = num + w * parts[s, :, :D].astype(F32)
    att = (num / den).astype(BF16)
    for t in range(2):
        for g in range(4):
            piece = att[:, t * 512 + g * PAIR : t * 512 + (g + 1) * PAIR]
            for d in range(PEERS):
                out[d, t * 64 + g * 16 : t * 64 + (g + 1) * 16, :] = piece


def merge(parts):
    return pl.pallas_call(
        merge_body,
        out_shape=jax.ShapeDtypeStruct((PEERS, 128, PAIR), BF16),
        in_specs=[IN_VMEM],
        out_specs=IN_VMEM,
        compiler_params=pltpu.CompilerParams(vmem_limit_bytes=16 * MIB),
        cost_estimate=pl.CostEstimate(
            flops=2 * 128 * 128 * D, bytes_accessed=1 * MIB, transcendentals=128 * D
        ),
        name="merge",
    )(parts)


def gather_blocks(tiling, lat, blocks, att):
    role = my_role()
    square = jnp.zeros((LATENTS, PAIR), F32)
    for k, block in enumerate(blocks):
        start = pl.multiple_of((role ^ k) * PAIR, PAIR)
        a = block[...]
        att[:, pl.ds(start, PAIR)] = a
        e = lat[:, pl.ds(start + tiling * 512, PAIR)].astype(F32) + a.astype(F32)
        square = square + e * e
    return square


def half_body(lat, a0, a1, a2, a3, wk, wv, pk, pv, sk, sv, square, att):
    square[...] = gather_blocks(0, lat, (a0, a1, a2, a3), att)
    sk[...] = pk[...] + dot(att[...], wk[:512, :])
    sv[...] = pv[...] + dot(att[...], wv[:512, :])


def add_half(latents, blocks, wk, wv, pk, pv):
    return pl.pallas_call(
        half_body,
        out_shape=[
            jax.ShapeDtypeStruct((LATENTS, D), F32),
            jax.ShapeDtypeStruct((LATENTS, D), F32),
            jax.ShapeDtypeStruct((LATENTS, PAIR), F32),
        ],
        in_specs=[IN_VMEM] * 9,
        out_specs=[IN_VMEM] * 3,
        scratch_shapes=[pltpu.VMEM((LATENTS, 512), BF16)],
        input_output_aliases={7: 0, 8: 1},
        compiler_params=pltpu.CompilerParams(vmem_limit_bytes=24 * MIB),
        cost_estimate=pl.CostEstimate(
            flops=2 * LATENTS * D * D, bytes_accessed=4 * MIB, transcendentals=0
        ),
        name="add_half",
    )(latents, *blocks, wk, wv, pk, pv)


def decode_body(lat, a0, a1, a2, a3, wk, wv, sk, sv, square, q, tok, out, att, lk, lv):
    total_square = square[...] + gather_blocks(1, lat, (a0, a1, a2, a3), att)
    mean_square = jnp.sum(total_square, axis=1, keepdims=True) * (1.0 / D)
    scale = lax.rsqrt(mean_square + 1e-06)
    lk[...] = ((sk[...] + dot(att[...], wk[512:, :])) * scale).astype(BF16)
    lv[...] = ((sv[...] + dot(att[...], wv[512:, :])) * scale).astype(BF16)
    left = left_half((ROWS, PAIR))
    for p in range(HEADS // 2):
        cols = slice(p * PAIR, (p + 1) * PAIR)
        scores = dot_t(both_heads(q[:, cols]), lk[:, cols])
        peak = jnp.max(scores, axis=1, keepdims=True)
        weights = jnp.exp2((scores - peak) * EXP2_SCALE)
        total = jnp.sum(weights, axis=1, keepdims=True)
        summed = dot(weights.astype(BF16), lv[:, cols])
        both = jnp.where(left, summed[:ROWS], summed[ROWS:]) / jnp.where(
            left, total[:ROWS], total[ROWS:]
        )
        out[:, cols] = (tok[:, cols].astype(F32) + both).astype(BF16)


def decode(latents, blocks, wk, wv, sk, sv, square, queries, tokens):
    return pl.pallas_call(
        decode_body,
        out_shape=jax.ShapeDtypeStruct((ROWS, D), BF16),
        in_specs=[IN_VMEM] * 12,
        out_specs=IN_VMEM,
        scratch_shapes=[
            pltpu.VMEM((LATENTS, 512), BF16),
            pltpu.VMEM((LATENTS, D), BF16),
            pltpu.VMEM((LATENTS, D), BF16),
        ],
        compiler_params=pltpu.CompilerParams(vmem_limit_bytes=32 * MIB),
        cost_estimate=pl.CostEstimate(
            flops=2 * LATENTS * D * D + 4 * ROWS * LATENTS * D,
            bytes_accessed=8 * MIB,
            transcendentals=ROWS * LATENTS * HEADS,
        ),
        name="decode",
    )(latents, *blocks, wk, wv, sk, sv, square, queries, tokens)


def per_device(
    tokens,
    valid_count,
    latents,
    key_weight,
    value_weight,
    query_weight,
    latent_key_weight,
    latent_value_weight,
):
    group = ("zh", "xh")
    kv = project_kv(tokens, key_weight, value_weight)
    kvs = ([kv[0]] + [None] * 3, [kv[4]] + [None] * 3)
    for t in range(2):
        for k in (3, 1, 2):
            kvs[t][k] = send(kv[4 * t + k], k, t)
    queries, pk, pv = prepare(
        tokens, latents, query_weight, latent_key_weight, latent_value_weight
    )
    first = attend(0, valid_count, latents, kvs[0])
    (partial,) = attend(1, valid_count, latents, kvs[1], first)
    parts = lax.all_to_all(partial, group, 0, 0, tiled=True)
    merged = merge(parts)
    rows = lax.all_to_all(merged, group, 0, 0, tiled=True)
    blocks = []
    for t in range(2):
        own = rows[:, t * 64 : (t + 1) * 64].reshape(LATENTS, PAIR)
        blocks.append([own, None, None, None])
        for k in (3, 1, 2):
            blocks[t][k] = send(own, k, t)
    sk, sv, square = add_half(
        latents, blocks[0], latent_key_weight, latent_value_weight, pk, pv
    )
    return decode(
        latents, blocks[1], latent_key_weight, latent_value_weight, sk, sv, square, queries, tokens
    )


def solution(mesh):
    split = Mesh(mesh.devices.reshape(NZ // 2, 2, NX // 2, 2, -1), (*AXES, "reg"))
    spread = P(("reg", *AXES), None)
    placed = (spread, P("reg"), P(), P(), P(), P(), P(), P())
    return jax.shard_map(
        per_device, mesh=split, in_specs=placed, out_specs=spread, check_vma=False
    )
```

```python
import functools
import math

import jax
import jax.numpy as jnp
from jax import lax
from jax.experimental import pallas as pl
from jax.experimental.pallas import tpu as pltpu
from jax.sharding import Mesh, PartitionSpec as P

D = 1024
HEADS = 16
LATENTS = 512
ROWS = 256
NX = 4
NZ = 8
PEERS = 8
PAIR = 128
SCALE = 0.125
EXP2_SCALE = SCALE * math.log2(math.e)
MIB = 1024 * 1024
KV_LIMIT = 16384


F32 = jnp.float32
BF16 = jnp.bfloat16
AXES = ("zh", "zl", "xh", "xl")
IN_VMEM = pl.BlockSpec(memory_space=pltpu.VMEM)
IN_HBM = pl.BlockSpec(memory_space=pltpu.HBM)
IN_SMEM = pl.BlockSpec(memory_space=pltpu.SMEM)


def dot(a, b):
    return jnp.dot(a, b, preferred_element_type=F32)


def dot_t(a, b):
    return lax.dot_general(a, b, (((1,), (1,)), ((), ())), preferred_element_type=F32)


def left_half(shape):
    return lax.broadcasted_iota(jnp.int32, shape, 1) < 64


def both_heads(pair):
    left = left_half(pair.shape)
    zero = jnp.zeros_like(pair)
    return jnp.concatenate([jnp.where(left, pair, zero), jnp.where(left, zero, pair)], axis=0)


def my_role():
    return lax.axis_index("zl") * 2 + lax.axis_index("xl")


def square_peer(z, x, k, tiling):
    if tiling == 0:
        return z ^ (k >> 1), x ^ (k & 1)
    dz = (2 * (z & 1) - 1) * (k >> 1)
    dx = (2 * (x & 1) - 1) * (k & 1)
    return (z + dz) & (NZ - 1), (x + dx) & (NX - 1)


def send(value, k, tiling):
    pairs = []
    for z in range(NZ):
        for x in range(NX):
            pz, px = square_peer(z, x, k, tiling)
            pairs.append((z * NX + x, pz * NX + px))
    return lax.ppermute(value, AXES, pairs)


def kv_body(tok_hbm, wk_hbm, wv_hbm, *refs):
    outs, (tok, wk, wv, acc, keys, values, tok_sem, w_sem) = refs[:8], refs[8:]
    half = D // 2
    tok_copy = pltpu.make_async_copy(tok_hbm, tok, tok_sem)
    copies = []
    for n in range(2):
        rows = pl.ds(n * half, half)
        for j, (hbm, vmem) in enumerate(((wk_hbm, wk), (wv_hbm, wv))):
            copies.append(pltpu.make_async_copy(hbm.at[rows], vmem.at[rows], w_sem.at[n, j]))
    tok_copy.start()
    for c in copies:
        c.start()
    tok_copy.wait()
    for j, w in enumerate((wk, wv)):
        copies[j].wait()
        acc[j] = dot(tok[:, :half], w[:half])
    for j, (w, result) in enumerate(((wk, keys), (wv, values))):
        copies[2 + j].wait()
        result[...] = (acc[j] + dot(tok[:, half:], w[half:])).astype(BF16)
    role = my_role()
    for k in range(4):
        start = pl.multiple_of((role ^ k) * PAIR, PAIR)
        for t in range(2):
            outs[4 * t + k][:, :PAIR] = keys[:, pl.ds(t * half + start, PAIR)]
            outs[4 * t + k][:, PAIR:] = values[:, pl.ds(t * half + start, PAIR)]


def project_kv(tokens, key_weight, value_weight):
    return pl.pallas_call(
        kv_body,
        out_shape=[jax.ShapeDtypeStruct((ROWS, 2 * PAIR), BF16)] * 8,
        in_specs=[IN_HBM] * 3,
        out_specs=[IN_VMEM] * 8,
        scratch_shapes=[
            pltpu.VMEM((ROWS, D), BF16),
            pltpu.VMEM((D, D), BF16),
            pltpu.VMEM((D, D), BF16),
            pltpu.VMEM((2, ROWS, D), F32),
            pltpu.VMEM((ROWS, D), BF16),
            pltpu.VMEM((ROWS, D), BF16),
            pltpu.SemaphoreType.DMA(()),
            pltpu.SemaphoreType.DMA((2, 2)),
        ],
        compiler_params=pltpu.CompilerParams(vmem_limit_bytes=KV_LIMIT * 1024),
        cost_estimate=pl.CostEstimate(
            flops=4 * ROWS * D * D, bytes_accessed=6 * MIB, transcendentals=0
        ),
        name="kv_proj",
    )(*[pltpu.with_memory_space_constraint(a, pltpu.HBM) for a in (tokens, key_weight, value_weight)])


def query_body(tok, wq, q):
    q[...] = dot(tok[...], wq[...]).astype(BF16)


def project_queries(tokens, query_weight):
    return pl.pallas_call(
        query_body,
        out_shape=jax.ShapeDtypeStruct((ROWS, D), BF16),
        in_specs=[IN_VMEM] * 2,
        out_specs=IN_VMEM,
        compiler_params=pltpu.CompilerParams(vmem_limit_bytes=8 * MIB),
        cost_estimate=pl.CostEstimate(
            flops=2 * ROWS * D * D, bytes_accessed=3 * MIB, transcendentals=0
        ),
        name="q_proj",
    )(tokens, query_weight)


def prepare_body(lat, wk, wv, pk, pv):
    pk[...] = dot(lat[...], wk[...])
    pv[...] = dot(lat[...], wv[...])


def prepare(latents, wk, wv):
    return pl.pallas_call(
        prepare_body,
        out_shape=[jax.ShapeDtypeStruct((LATENTS, D), F32)] * 2,
        in_specs=[IN_VMEM] * 3,
        out_specs=[IN_VMEM] * 2,
        compiler_params=pltpu.CompilerParams(vmem_limit_bytes=20 * MIB),
        cost_estimate=pl.CostEstimate(
            flops=4 * LATENTS * D * D, bytes_accessed=9 * MIB, transcendentals=0
        ),
        name="prepare",
    )(latents, wk, wv)


def attend_body(tiling, count, lat, kv0, kv1, kv2, kv3, *refs):
    if tiling == 0:
        out, stat_out = refs
    else:
        first, first_stats, out = refs
    z = lax.axis_index("zh") * 2 + lax.axis_index("zl")
    x = lax.axis_index("xh") * 2 + lax.axis_index("xl")
    chunks = (kv0, kv1, kv2, kv3)
    lane = lax.broadcasted_iota(jnp.int32, (1, ROWS), 1)
    valid = []
    for k in range(4):
        pz, px = square_peer(z, x, k, tiling)
        valid.append((pz * NX + px) * ROWS + lane < count[0])
    start = pl.multiple_of(my_role() * PAIR, PAIR) + tiling * 512
    block = 256
    for b in range(LATENTS // block):
        rows = slice(b * block, (b + 1) * block)
        query = both_heads(lat[rows, pl.ds(start, PAIR)])
        scores = [jnp.where(valid[k], dot_t(query, chunks[k][:, :PAIR]), -1e30) for k in range(4)]
        top = jnp.maximum(jnp.maximum(scores[0], scores[1]), jnp.maximum(scores[2], scores[3]))
        peak = jnp.maximum(jnp.max(top, axis=1, keepdims=True), -1e29)
        weights = [jnp.exp2((s - peak) * EXP2_SCALE) for s in scores]
        total = jnp.sum((weights[0] + weights[1]) + (weights[2] + weights[3]), axis=1, keepdims=True)
        total = jnp.maximum(total, 1.0)
        summed = sum(dot(weights[k].astype(BF16), chunks[k][:, PAIR:]) for k in range(4))
        lse = peak * SCALE + jnp.log(total)
        left = left_half((block, PAIR))
        means = jnp.where(left, summed[:block], summed[block:]) / jnp.where(
            left, total[:block], total[block:]
        )
        means = means.astype(BF16)
        stat_lane = lax.broadcasted_iota(jnp.int32, (block, 128), 1)
        stat_row = lax.broadcasted_iota(jnp.int32, (block, 128), 0)
        place = stat_lane - ((stat_row >> 4) & 3) * 4
        stats = jnp.zeros((block, 128), F32) if tiling == 0 else first_stats[rows, :]
        for hh in range(2):
            rest = lse[hh * block : (hh + 1) * block]
            for piece in range(3):
                part = rest.astype(BF16).astype(F32)
                rest = rest - part
                stats = jnp.where(place == piece * 16 + 2 * tiling + hh, part, stats)
        if tiling == 0:
            stat_out[rows, :] = stats
        for d in range(block // 64):
            dest = b * (block // 64) + d
            for g in range(4):
                part = means[d * 64 + g * 16 : d * 64 + (g + 1) * 16, :]
                if tiling == 0:
                    out[dest, :, g * PAIR : (g + 1) * PAIR] = part
                else:
                    out[dest, :, 512 + g * PAIR : 512 + (g + 1) * PAIR] = part
            if tiling == 1:
                out[dest, :, :512] = first[dest]
                keep = stats[d * 64 : d * 64 + 16]
                for g in range(1, 4):
                    keep = keep + stats[d * 64 + g * 16 : d * 64 + (g + 1) * 16]
                out[dest, :, D : D + 128] = keep.astype(BF16)


def attend(tiling, count, latents, kvs, first=()):
    if tiling == 0:
        out_shape = [
            jax.ShapeDtypeStruct((PEERS, 16, 512), BF16),
            jax.ShapeDtypeStruct((LATENTS, 128), F32),
        ]
    else:
        out_shape = [jax.ShapeDtypeStruct((PEERS, 16, D + 128), BF16)]
    return pl.pallas_call(
        functools.partial(attend_body, tiling),
        out_shape=out_shape,
        in_specs=[IN_SMEM] + [IN_VMEM] * (5 + len(first)),
        out_specs=[IN_VMEM] * len(out_shape),
        compiler_params=pltpu.CompilerParams(vmem_limit_bytes=24 * MIB),
        cost_estimate=pl.CostEstimate(
            flops=4 * LATENTS * ROWS * 4 * PAIR,
            bytes_accessed=1 * MIB,
            transcendentals=LATENTS * ROWS * 8,
        ),
        name="attend",
    )(count, latents, *kvs, *first)


def merge_body(parts, out):
    stats = parts[:, :, D : D + 128].reshape(PEERS * 16, 128)
    j = lax.broadcasted_iota(jnp.int32, (128, D), 0)
    n = lax.broadcasted_iota(jnp.int32, (128, D), 1)
    head = ((n >> 7) & 3) * 4 + (n >> 9) * 2 + ((n >> 6) & 1)
    spread = jnp.where(((j & 15) == head) & (j < 48), 1.0, 0.0).astype(BF16)
    lse = dot(stats, spread).reshape(PEERS, 16, D)
    peak = jnp.max(lse, axis=0)
    num = jnp.zeros((16, D), F32)
    den = jnp.zeros((16, D), F32)
    for s in range(PEERS):
        w = jnp.exp(lse[s] - peak)
        den = den + w
        num = num + w * parts[s, :, :D].astype(F32)
    att = (num / den).astype(BF16)
    for t in range(2):
        for g in range(4):
            piece = att[:, t * 512 + g * PAIR : t * 512 + (g + 1) * PAIR]
            for d in range(PEERS):
                out[d, t * 64 + g * 16 : t * 64 + (g + 1) * 16, :] = piece


def merge(parts):
    return pl.pallas_call(
        merge_body,
        out_shape=jax.ShapeDtypeStruct((PEERS, 128, PAIR), BF16),
        in_specs=[IN_VMEM],
        out_specs=IN_VMEM,
        compiler_params=pltpu.CompilerParams(vmem_limit_bytes=16 * MIB),
        cost_estimate=pl.CostEstimate(
            flops=2 * 128 * 128 * D, bytes_accessed=1 * MIB, transcendentals=128 * D
        ),
        name="merge",
    )(parts)


def gather_blocks(tiling, lat, blocks, att):
    role = my_role()
    square = jnp.zeros((LATENTS, PAIR), F32)
    for k, block in enumerate(blocks):
        start = pl.multiple_of((role ^ k) * PAIR, PAIR)
        a = block[...]
        att[:, pl.ds(start, PAIR)] = a
        e = lat[:, pl.ds(start + tiling * 512, PAIR)].astype(F32) + a.astype(F32)
        square = square + e * e
    return square


def half_body(lat, a0, a1, a2, a3, wk, wv, pk, pv, sk, sv, square, att):
    square[...] = gather_blocks(0, lat, (a0, a1, a2, a3), att)
    sk[...] = pk[...] + dot(att[...], wk[:512, :])
    sv[...] = pv[...] + dot(att[...], wv[:512, :])


def add_half(latents, blocks, wk, wv, pk, pv):
    return pl.pallas_call(
        half_body,
        out_shape=[
            jax.ShapeDtypeStruct((LATENTS, D), F32),
            jax.ShapeDtypeStruct((LATENTS, D), F32),
            jax.ShapeDtypeStruct((LATENTS, PAIR), F32),
        ],
        in_specs=[IN_VMEM] * 9,
        out_specs=[IN_VMEM] * 3,
        scratch_shapes=[pltpu.VMEM((LATENTS, 512), BF16)],
        input_output_aliases={7: 0, 8: 1},
        compiler_params=pltpu.CompilerParams(vmem_limit_bytes=24 * MIB),
        cost_estimate=pl.CostEstimate(
            flops=2 * LATENTS * D * D, bytes_accessed=4 * MIB, transcendentals=0
        ),
        name="add_half",
    )(latents, *blocks, wk, wv, pk, pv)


def decode_body(lat, a0, a1, a2, a3, wk, wv, sk, sv, square, q, tok, out, att, lk, lv):
    total_square = square[...] + gather_blocks(1, lat, (a0, a1, a2, a3), att)
    mean_square = jnp.sum(total_square, axis=1, keepdims=True) * (1.0 / D)
    scale = lax.rsqrt(mean_square + 1e-06)
    lk[...] = ((sk[...] + dot(att[...], wk[512:, :])) * scale).astype(BF16)
    lv[...] = ((sv[...] + dot(att[...], wv[512:, :])) * scale).astype(BF16)
    left = left_half((ROWS, PAIR))
    for p in range(HEADS // 2):
        cols = slice(p * PAIR, (p + 1) * PAIR)
        scores = dot_t(both_heads(q[:, cols]), lk[:, cols])
        peak = jnp.max(scores, axis=1, keepdims=True)
        weights = jnp.exp2((scores - peak) * EXP2_SCALE)
        total = jnp.sum(weights, axis=1, keepdims=True)
        summed = dot(weights.astype(BF16), lv[:, cols])
        both = jnp.where(left, summed[:ROWS], summed[ROWS:]) / jnp.where(
            left, total[:ROWS], total[ROWS:]
        )
        out[:, cols] = (tok[:, cols].astype(F32) + both).astype(BF16)


def decode(latents, blocks, wk, wv, sk, sv, square, queries, tokens):
    return pl.pallas_call(
        decode_body,
        out_shape=jax.ShapeDtypeStruct((ROWS, D), BF16),
        in_specs=[IN_VMEM] * 12,
        out_specs=IN_VMEM,
        scratch_shapes=[
            pltpu.VMEM((LATENTS, 512), BF16),
            pltpu.VMEM((LATENTS, D), BF16),
            pltpu.VMEM((LATENTS, D), BF16),
        ],
        compiler_params=pltpu.CompilerParams(vmem_limit_bytes=32 * MIB),
        cost_estimate=pl.CostEstimate(
            flops=2 * LATENTS * D * D + 4 * ROWS * LATENTS * D,
            bytes_accessed=8 * MIB,
            transcendentals=ROWS * LATENTS * HEADS,
        ),
        name="decode",
    )(latents, *blocks, wk, wv, sk, sv, square, queries, tokens)


def per_device(
    tokens,
    valid_count,
    latents,
    key_weight,
    value_weight,
    query_weight,
    latent_key_weight,
    latent_value_weight,
):
    group = ("zh", "xh")
    kv = project_kv(tokens, key_weight, value_weight)
    kvs = ([kv[0]] + [None] * 3, [kv[4]] + [None] * 3)
    for t in range(2):
        for k in (3, 1, 2):
            kvs[t][k] = send(kv[4 * t + k], k, t)
    queries = project_queries(tokens, query_weight)
    kvs[0][0], queries = lax.optimization_barrier((kvs[0][0], queries))
    pk, pv = prepare(latents, latent_key_weight, latent_value_weight)
    first = attend(0, valid_count, latents, kvs[0])
    (partial,) = attend(1, valid_count, latents, kvs[1], first)
    parts = lax.all_to_all(partial, group, 0, 0, tiled=True)
    merged = merge(parts)
    rows = lax.all_to_all(merged, group, 0, 0, tiled=True)
    blocks = []
    for t in range(2):
        own = rows[:, t * 64 : (t + 1) * 64].reshape(LATENTS, PAIR)
        blocks.append([own, None, None, None])
        for k in (3, 1, 2):
            blocks[t][k] = send(own, k, t)
    sk, sv, square = add_half(
        latents, blocks[0], latent_key_weight, latent_value_weight, pk, pv
    )
    return decode(
        latents, blocks[1], latent_key_weight, latent_value_weight, sk, sv, square, queries, tokens
    )


def solution(mesh):
    split = Mesh(mesh.devices.reshape(NZ // 2, 2, NX // 2, 2, -1), (*AXES, "reg"))
    spread = P(("reg", *AXES), None)
    placed = (spread, P("reg"), P(), P(), P(), P(), P(), P())
    return jax.shard_map(
        per_device, mesh=split, in_specs=placed, out_specs=spread, check_vma=False
    )
```

```python
import functools
import math

import jax
import jax.numpy as jnp
from jax import lax
from jax.experimental import pallas as pl
from jax.experimental.pallas import tpu as pltpu
from jax.sharding import Mesh, PartitionSpec as P

D = 1024
HEADS = 16
LATENTS = 512
ROWS = 256
NX = 4
NZ = 8
PEERS = 8
PAIR = 128
SCALE = 0.125
EXP2_SCALE = SCALE * math.log2(math.e)
MIB = 1024 * 1024
KV_LIMIT = 16384


F32 = jnp.float32
BF16 = jnp.bfloat16
AXES = ("zh", "zl", "xh", "xl")
IN_VMEM = pl.BlockSpec(memory_space=pltpu.VMEM)
IN_HBM = pl.BlockSpec(memory_space=pltpu.HBM)
IN_SMEM = pl.BlockSpec(memory_space=pltpu.SMEM)


def dot(a, b):
    return jnp.dot(a, b, preferred_element_type=F32)


def dot_t(a, b):
    return lax.dot_general(a, b, (((1,), (1,)), ((), ())), preferred_element_type=F32)


def left_half(shape):
    return lax.broadcasted_iota(jnp.int32, shape, 1) < 64


def both_heads(pair):
    left = left_half(pair.shape)
    zero = jnp.zeros_like(pair)
    return jnp.concatenate([jnp.where(left, pair, zero), jnp.where(left, zero, pair)], axis=0)


def my_role():
    return lax.axis_index("zl") * 2 + lax.axis_index("xl")


def square_peer(z, x, k, tiling):
    if tiling == 0:
        return z ^ (k >> 1), x ^ (k & 1)
    dz = (2 * (z & 1) - 1) * (k >> 1)
    dx = (2 * (x & 1) - 1) * (k & 1)
    return (z + dz) & (NZ - 1), (x + dx) & (NX - 1)


def send(value, k, tiling):
    pairs = []
    for z in range(NZ):
        for x in range(NX):
            pz, px = square_peer(z, x, k, tiling)
            pairs.append((z * NX + x, pz * NX + px))
    return lax.ppermute(value, AXES, pairs)


def kv_body(tok_hbm, wk_hbm, wv_hbm, *refs):
    outs, (tok, wk, wv, acc, keys, values, tok_sem, w_sem) = refs[:8], refs[8:]
    half = D // 2
    tok_copy = pltpu.make_async_copy(tok_hbm, tok, tok_sem)
    copies = []
    for n in range(2):
        rows = pl.ds(n * half, half)
        for j, (hbm, vmem) in enumerate(((wk_hbm, wk), (wv_hbm, wv))):
            copies.append(pltpu.make_async_copy(hbm.at[rows], vmem.at[rows], w_sem.at[n, j]))
    tok_copy.start()
    for c in copies:
        c.start()
    tok_copy.wait()
    for j, w in enumerate((wk, wv)):
        copies[j].wait()
        acc[j] = dot(tok[:, :half], w[:half])
    for j, (w, result) in enumerate(((wk, keys), (wv, values))):
        copies[2 + j].wait()
        result[...] = (acc[j] + dot(tok[:, half:], w[half:])).astype(BF16)
    role = my_role()
    for k in range(4):
        start = pl.multiple_of((role ^ k) * PAIR, PAIR)
        for t in range(2):
            outs[4 * t + k][:, :PAIR] = keys[:, pl.ds(t * half + start, PAIR)]
            outs[4 * t + k][:, PAIR:] = values[:, pl.ds(t * half + start, PAIR)]


def project_kv(tokens, key_weight, value_weight):
    return pl.pallas_call(
        kv_body,
        out_shape=[jax.ShapeDtypeStruct((ROWS, 2 * PAIR), BF16)] * 8,
        in_specs=[IN_HBM] * 3,
        out_specs=[IN_VMEM] * 8,
        scratch_shapes=[
            pltpu.VMEM((ROWS, D), BF16),
            pltpu.VMEM((D, D), BF16),
            pltpu.VMEM((D, D), BF16),
            pltpu.VMEM((2, ROWS, D), F32),
            pltpu.VMEM((ROWS, D), BF16),
            pltpu.VMEM((ROWS, D), BF16),
            pltpu.SemaphoreType.DMA(()),
            pltpu.SemaphoreType.DMA((2, 2)),
        ],
        compiler_params=pltpu.CompilerParams(vmem_limit_bytes=KV_LIMIT * 1024),
        cost_estimate=pl.CostEstimate(
            flops=4 * ROWS * D * D, bytes_accessed=6 * MIB, transcendentals=0
        ),
        name="kv_proj",
    )(*[pltpu.with_memory_space_constraint(a, pltpu.HBM) for a in (tokens, key_weight, value_weight)])


def query_body(tok, wq, q):
    q[...] = dot(tok[...], wq[...]).astype(BF16)


def project_queries(tokens, query_weight):
    return pl.pallas_call(
        query_body,
        out_shape=jax.ShapeDtypeStruct((ROWS, D), BF16),
        in_specs=[IN_VMEM] * 2,
        out_specs=IN_VMEM,
        compiler_params=pltpu.CompilerParams(vmem_limit_bytes=8 * MIB),
        cost_estimate=pl.CostEstimate(
            flops=2 * ROWS * D * D, bytes_accessed=3 * MIB, transcendentals=0
        ),
        name="q_proj",
    )(tokens, query_weight)


def attend_body(tiling, count, lat, kv0, kv3, kv1, kv2, *refs):
    if tiling == 0:
        out, stat_out = refs
    else:
        first, first_stats, out = refs
    z = lax.axis_index("zh") * 2 + lax.axis_index("zl")
    x = lax.axis_index("xh") * 2 + lax.axis_index("xl")
    chunks = (kv0, kv1, kv2, kv3)
    lane = lax.broadcasted_iota(jnp.int32, (1, ROWS), 1)
    valid = []
    for k in range(4):
        pz, px = square_peer(z, x, k, tiling)
        valid.append((pz * NX + px) * ROWS + lane < count[0])
    start = pl.multiple_of(my_role() * PAIR, PAIR) + tiling * 512
    block = 256
    stat_lane = lax.broadcasted_iota(jnp.int32, (block, 128), 1)
    stat_row = lax.broadcasted_iota(jnp.int32, (block, 128), 0)
    odd = (stat_lane & 1) == 1
    piece = stat_lane >> 4
    mine = (((stat_lane & 15) >> 1) == ((stat_row >> 4) & 3) * 2 + tiling) & (piece < 3)
    for b in range(LATENTS // block):
        rows = slice(b * block, (b + 1) * block)
        query = both_heads(lat[rows, pl.ds(start, PAIR)])
        scores = [jnp.where(valid[k], dot_t(query, chunks[k][:, :PAIR]), -1e30) for k in range(4)]
        top = jnp.maximum(jnp.maximum(scores[0], scores[1]), jnp.maximum(scores[2], scores[3]))
        peak = jnp.maximum(jnp.max(top, axis=1, keepdims=True), -1e29)
        weights = [jnp.exp2((s - peak) * EXP2_SCALE) for s in scores]
        total = jnp.sum((weights[0] + weights[1]) + (weights[2] + weights[3]), axis=1, keepdims=True)
        total = jnp.maximum(total, 1.0)
        summed = sum(dot(weights[k].astype(BF16), chunks[k][:, PAIR:]) for k in range(4))
        left = left_half((block, PAIR))
        means = jnp.where(left, summed[:block], summed[block:]) / jnp.where(
            left, total[:block], total[block:]
        )
        means = means.astype(BF16)
        lse = jnp.where(odd, peak[block:], peak[:block]) * SCALE + jnp.log(
            jnp.where(odd, total[block:], total[:block])
        )
        high = lse.astype(BF16).astype(F32)
        rest = lse - high
        middle = rest.astype(BF16).astype(F32)
        stats = jnp.where(piece == 0, high, jnp.where(piece == 1, middle, rest - middle))
        stats = jnp.where(mine, stats, 0.0 if tiling == 0 else first_stats[rows, :])
        if tiling == 0:
            stat_out[rows, :] = stats
        for d in range(block // 64):
            dest = b * (block // 64) + d
            for g in range(4):
                part = means[d * 64 + g * 16 : d * 64 + (g + 1) * 16, :]
                if tiling == 0:
                    out[dest, :, g * PAIR : (g + 1) * PAIR] = part
                else:
                    out[dest, :, 512 + g * PAIR : 512 + (g + 1) * PAIR] = part
            if tiling == 1:
                out[dest, :, :512] = first[dest]
                keep = stats[d * 64 : d * 64 + 16]
                for g in range(1, 4):
                    keep = keep + stats[d * 64 + g * 16 : d * 64 + (g + 1) * 16]
                out[dest, :, D : D + 128] = keep.astype(BF16)


def attend(tiling, count, latents, kvs, first=()):
    if tiling == 0:
        out_shape = [
            jax.ShapeDtypeStruct((PEERS, 16, 512), BF16),
            jax.ShapeDtypeStruct((LATENTS, 128), F32),
        ]
    else:
        out_shape = [jax.ShapeDtypeStruct((PEERS, 16, D + 128), BF16)]
    return pl.pallas_call(
        functools.partial(attend_body, tiling),
        out_shape=out_shape,
        in_specs=[IN_SMEM] + [IN_VMEM] * (5 + len(first)),
        out_specs=[IN_VMEM] * len(out_shape),
        compiler_params=pltpu.CompilerParams(vmem_limit_bytes=24 * MIB),
        cost_estimate=pl.CostEstimate(
            flops=4 * LATENTS * ROWS * 4 * PAIR,
            bytes_accessed=1 * MIB,
            transcendentals=LATENTS * ROWS * 8,
        ),
        name="attend",
    )(count, latents, kvs[0], kvs[3], kvs[1], kvs[2], *first)


def merge_body(parts, out):
    stats = parts[:, :, D : D + 128].reshape(PEERS * 16, 128)
    j = lax.broadcasted_iota(jnp.int32, (128, D), 0)
    n = lax.broadcasted_iota(jnp.int32, (128, D), 1)
    head = ((n >> 7) & 3) * 4 + (n >> 9) * 2 + ((n >> 6) & 1)
    spread = jnp.where(((j & 15) == head) & (j < 48), 1.0, 0.0).astype(BF16)
    lse = dot(stats, spread).reshape(PEERS, 16, D)
    peak = jnp.max(lse, axis=0)
    num = jnp.zeros((16, D), F32)
    den = jnp.zeros((16, D), F32)
    for s in range(PEERS):
        w = jnp.exp(lse[s] - peak)
        den = den + w
        num = num + w * parts[s, :, :D].astype(F32)
    att = (num / den).astype(BF16)
    for t in range(2):
        for g in range(4):
            piece = att[:, t * 512 + g * PAIR : t * 512 + (g + 1) * PAIR]
            for d in range(PEERS):
                out[d, t * 64 + g * 16 : t * 64 + (g + 1) * 16, :] = piece


def merge(parts):
    return pl.pallas_call(
        merge_body,
        out_shape=jax.ShapeDtypeStruct((PEERS, 128, PAIR), BF16),
        in_specs=[IN_VMEM],
        out_specs=IN_VMEM,
        compiler_params=pltpu.CompilerParams(vmem_limit_bytes=16 * MIB),
        cost_estimate=pl.CostEstimate(
            flops=2 * 128 * 128 * D, bytes_accessed=1 * MIB, transcendentals=128 * D
        ),
        name="merge",
    )(parts)


def half_attention(flipped, lat, same, other, wk, wv, q, enc, lk, lv):
    rows = lax.axis_index("xh") ^ flipped
    xl = lax.axis_index("xl")
    for zh in range(4):
        where = pl.multiple_of((zh * 2 + rows) * 64, 64)
        for zl in range(2):
            for t in range(2):
                for block, low in ((same, xl), (other, 1 - xl)):
                    col = pl.multiple_of((2 * zl + low) * PAIR, PAIR) + t * 512
                    enc[zh * 64 : (zh + 1) * 64, pl.ds(col, PAIR)] = lat[
                        pl.ds(where, 64), pl.ds(col, PAIR)
                    ].astype(F32) + block[2 * zh + zl, t * 64 : (t + 1) * 64, :].astype(F32)
    encoded = enc[...]
    square = jnp.sum(encoded * encoded, axis=1, keepdims=True)
    normed = (encoded * lax.rsqrt(square * (1.0 / D) + 1e-06)).astype(BF16)
    lk[...] = dot(normed, wk[...]).astype(BF16)
    lv[...] = dot(normed, wv[...]).astype(BF16)
    left = left_half((ROWS, PAIR))
    for p in range(HEADS // 2):
        cols = slice(p * PAIR, (p + 1) * PAIR)
        scores = dot_t(both_heads(q[:, cols]), lk[:, cols])
        peak = jnp.max(scores, axis=1, keepdims=True)
        weights = jnp.exp2((scores - peak) * EXP2_SCALE)
        total = jnp.sum(weights, axis=1, keepdims=True)
        summed = dot(weights.astype(BF16), lv[:, cols])
        yield (
            cols,
            jnp.where(left, summed[:ROWS], summed[ROWS:]),
            jnp.where(left, peak[:ROWS], peak[ROWS:]),
            jnp.where(left, total[:ROWS], total[ROWS:]),
        )


def near_body(lat, same, other, wk, wv, q, summed_out, peak_out, total_out, enc, lk, lv):
    for cols, summed, peak, total in half_attention(0, lat, same, other, wk, wv, q, enc, lk, lv):
        summed_out[:, cols] = summed
        peak_out[:, cols] = peak
        total_out[:, cols] = total


def far_body(lat, same, other, wk, wv, q, summed_in, peak_in, total_in, tok, out, enc, lk, lv):
    for cols, summed, peak, total in half_attention(1, lat, same, other, wk, wv, q, enc, lk, lv):
        top = jnp.maximum(peak, peak_in[:, cols])
        here = jnp.exp2((peak - top) * EXP2_SCALE)
        there = jnp.exp2((peak_in[:, cols] - top) * EXP2_SCALE)
        num = summed * here + summed_in[:, cols] * there
        den = total * here + total_in[:, cols] * there
        out[:, cols] = (tok[:, cols].astype(F32) + num / den).astype(BF16)


DECODE_SCRATCH = [
    pltpu.VMEM((LATENTS // 2, D), F32),
    pltpu.VMEM((LATENTS // 2, D), BF16),
    pltpu.VMEM((LATENTS // 2, D), BF16),
]
DECODE_COST = pl.CostEstimate(
    flops=2 * LATENTS * D * D + 2 * ROWS * LATENTS * D,
    bytes_accessed=8 * MIB,
    transcendentals=ROWS * LATENTS * HEADS // 2,
)


def decode_near(latents, same, other, wk, wv, queries):
    return pl.pallas_call(
        near_body,
        out_shape=[jax.ShapeDtypeStruct((ROWS, D), F32)] * 3,
        in_specs=[IN_VMEM] * 6,
        out_specs=[IN_VMEM] * 3,
        scratch_shapes=DECODE_SCRATCH,
        compiler_params=pltpu.CompilerParams(vmem_limit_bytes=24 * MIB),
        cost_estimate=DECODE_COST,
        name="decode_near",
    )(latents, same, other, wk, wv, queries)


def decode_far(latents, same, other, wk, wv, queries, near, tokens):
    return pl.pallas_call(
        far_body,
        out_shape=jax.ShapeDtypeStruct((ROWS, D), BF16),
        in_specs=[IN_VMEM] * 10,
        out_specs=IN_VMEM,
        scratch_shapes=DECODE_SCRATCH,
        compiler_params=pltpu.CompilerParams(vmem_limit_bytes=24 * MIB),
        cost_estimate=DECODE_COST,
        name="decode_far",
    )(latents, same, other, wk, wv, queries, *near, tokens)


def send_x(value, flip):
    pairs = [(z * NX + x, z * NX + (x ^ flip)) for z in range(NZ) for x in range(NX)]
    return lax.ppermute(value, AXES, pairs)


def per_device(
    tokens,
    valid_count,
    latents,
    key_weight,
    value_weight,
    query_weight,
    latent_key_weight,
    latent_value_weight,
):
    kv = project_kv(tokens, key_weight, value_weight)
    kvs = ([kv[0]] + [None] * 3, [kv[4]] + [None] * 3)
    for t in range(2):
        for k in (3, 1, 2):
            kvs[t][k] = send(kv[4 * t + k], k, t)
    queries = project_queries(tokens, query_weight)
    kvs[0][0], queries = lax.optimization_barrier((kvs[0][0], queries))
    first = attend(0, valid_count, latents, kvs[0])
    (partial,) = attend(1, valid_count, latents, kvs[1], first)
    parts = lax.all_to_all(partial, ("zh", "xh"), 0, 0, tiled=True)
    merged = merge(parts)
    rows = lax.all_to_all(merged, ("zh", "zl"), 0, 0, tiled=True)
    blocks = [rows] + [send_x(rows, flip) for flip in (1, 2, 3)]
    near = decode_near(
        latents, blocks[0], blocks[1], latent_key_weight, latent_value_weight, queries
    )
    return decode_far(
        latents, blocks[2], blocks[3], latent_key_weight, latent_value_weight, queries, near, tokens
    )


def solution(mesh):
    split = Mesh(mesh.devices.reshape(NZ // 2, 2, NX // 2, 2, -1), (*AXES, "reg"))
    spread = P(("reg", *AXES), None)
    placed = (spread, P("reg"), P(), P(), P(), P(), P(), P())
    return jax.shard_map(
        per_device, mesh=split, in_specs=placed, out_specs=spread, check_vma=False
    )
```

```python
import functools
import math

import jax
import jax.numpy as jnp
from jax import lax
from jax.experimental import pallas as pl
from jax.experimental.pallas import tpu as pltpu
from jax.sharding import Mesh, PartitionSpec as P

D = 1024
HEADS = 16
LATENTS = 512
ROWS = 256
NX = 4
NZ = 8
PEERS = 8
PAIR = 128
SCALE = 0.125
EXP2_SCALE = SCALE * math.log2(math.e)
MIB = 1024 * 1024
KV_LIMIT = 16384
STAGGER_NS = 4000


F32 = jnp.float32
BF16 = jnp.bfloat16
AXES = ("zh", "zl", "xh", "xl")
IN_VMEM = pl.BlockSpec(memory_space=pltpu.VMEM)
IN_HBM = pl.BlockSpec(memory_space=pltpu.HBM)
IN_SMEM = pl.BlockSpec(memory_space=pltpu.SMEM)


def dot(a, b):
    return jnp.dot(a, b, preferred_element_type=F32)


def dot_t(a, b):
    return lax.dot_general(a, b, (((1,), (1,)), ((), ())), preferred_element_type=F32)


def left_half(shape):
    return lax.broadcasted_iota(jnp.int32, shape, 1) < 64


def both_heads(pair):
    left = left_half(pair.shape)
    zero = jnp.zeros_like(pair)
    return jnp.concatenate([jnp.where(left, pair, zero), jnp.where(left, zero, pair)], axis=0)


def my_role():
    return lax.axis_index("zl") * 2 + lax.axis_index("xl")


def square_peer(z, x, k, tiling):
    if tiling == 0:
        return z ^ (k >> 1), x ^ (k & 1)
    dz = (2 * (z & 1) - 1) * (k >> 1)
    dx = (2 * (x & 1) - 1) * (k & 1)
    return (z + dz) & (NZ - 1), (x + dx) & (NX - 1)


def send(value, k, tiling):
    pairs = []
    for z in range(NZ):
        for x in range(NX):
            pz, px = square_peer(z, x, k, tiling)
            pairs.append((z * NX + x, pz * NX + px))
    return lax.ppermute(value, AXES, pairs)


def kv_body(tok_hbm, wk_hbm, wv_hbm, *refs):
    outs, (tok, wk, wv, acc, keys, values, tok_sem, w_sem) = refs[:8], refs[8:]
    half = D // 2
    tok_copy = pltpu.make_async_copy(tok_hbm, tok, tok_sem)
    copies = []
    for n in range(2):
        rows = pl.ds(n * half, half)
        for j, (hbm, vmem) in enumerate(((wk_hbm, wk), (wv_hbm, wv))):
            copies.append(pltpu.make_async_copy(hbm.at[rows], vmem.at[rows], w_sem.at[n, j]))
    tok_copy.start()
    for c in copies:
        c.start()
    tok_copy.wait()
    for j, w in enumerate((wk, wv)):
        copies[j].wait()
        acc[j] = dot(tok[:, :half], w[:half])
    for j, (w, result) in enumerate(((wk, keys), (wv, values))):
        copies[2 + j].wait()
        result[...] = (acc[j] + dot(tok[:, half:], w[half:])).astype(BF16)
    role = my_role()
    for k in range(4):
        start = pl.multiple_of((role ^ k) * PAIR, PAIR)
        for t in range(2):
            outs[4 * t + k][:, :PAIR] = keys[:, pl.ds(t * half + start, PAIR)]
            outs[4 * t + k][:, PAIR:] = values[:, pl.ds(t * half + start, PAIR)]

    @pl.when(lax.rem(lax.axis_index("reg"), 2) == 1)
    def _():
        pl.delay(STAGGER_NS)


def project_kv(tokens, key_weight, value_weight):
    return pl.pallas_call(
        kv_body,
        out_shape=[jax.ShapeDtypeStruct((ROWS, 2 * PAIR), BF16)] * 8,
        in_specs=[IN_HBM] * 3,
        out_specs=[IN_VMEM] * 8,
        scratch_shapes=[
            pltpu.VMEM((ROWS, D), BF16),
            pltpu.VMEM((D, D), BF16),
            pltpu.VMEM((D, D), BF16),
            pltpu.VMEM((2, ROWS, D), F32),
            pltpu.VMEM((ROWS, D), BF16),
            pltpu.VMEM((ROWS, D), BF16),
            pltpu.SemaphoreType.DMA(()),
            pltpu.SemaphoreType.DMA((2, 2)),
        ],
        compiler_params=pltpu.CompilerParams(vmem_limit_bytes=KV_LIMIT * 1024),
        cost_estimate=pl.CostEstimate(
            flops=4 * ROWS * D * D, bytes_accessed=6 * MIB, transcendentals=0
        ),
        name="kv_proj",
    )(*[pltpu.with_memory_space_constraint(a, pltpu.HBM) for a in (tokens, key_weight, value_weight)])


def query_body(tok, wq, after, q):
    q[...] = dot(tok[...], wq[...]).astype(BF16)


def project_queries(tokens, query_weight, after):
    return pl.pallas_call(
        query_body,
        out_shape=jax.ShapeDtypeStruct((ROWS, D), BF16),
        in_specs=[IN_VMEM] * 2 + [pl.BlockSpec(memory_space=pl.ANY)],
        out_specs=IN_VMEM,
        compiler_params=pltpu.CompilerParams(vmem_limit_bytes=8 * MIB),
        cost_estimate=pl.CostEstimate(
            flops=2 * ROWS * D * D, bytes_accessed=3 * MIB, transcendentals=0
        ),
        name="q_proj",
    )(tokens, query_weight, after)


def attend_body(tiling, count, lat, kv0, kv3, kv1, kv2, *refs):
    if tiling == 0:
        out, stat_out = refs
    else:
        first, first_stats, out = refs
    z = lax.axis_index("zh") * 2 + lax.axis_index("zl")
    x = lax.axis_index("xh") * 2 + lax.axis_index("xl")
    chunks = (kv0, kv1, kv2, kv3)
    lane = lax.broadcasted_iota(jnp.int32, (1, ROWS), 1)
    valid = []
    for k in range(4):
        pz, px = square_peer(z, x, k, tiling)
        valid.append((pz * NX + px) * ROWS + lane < count[0])
    start = pl.multiple_of(my_role() * PAIR, PAIR) + tiling * 512
    block = 256
    stat_lane = lax.broadcasted_iota(jnp.int32, (block, 128), 1)
    stat_row = lax.broadcasted_iota(jnp.int32, (block, 128), 0)
    odd = (stat_lane & 1) == 1
    piece = stat_lane >> 4
    mine = (((stat_lane & 15) >> 1) == ((stat_row >> 4) & 3) * 2 + tiling) & (piece < 3)
    for b in range(LATENTS // block):
        rows = slice(b * block, (b + 1) * block)
        query = both_heads(lat[rows, pl.ds(start, PAIR)])
        scores = [jnp.where(valid[k], dot_t(query, chunks[k][:, :PAIR]), -1e30) for k in range(4)]
        top = jnp.maximum(jnp.maximum(scores[0], scores[1]), jnp.maximum(scores[2], scores[3]))
        peak = jnp.maximum(jnp.max(top, axis=1, keepdims=True), -1e29)
        weights = [jnp.exp2((s - peak) * EXP2_SCALE) for s in scores]
        total = jnp.sum((weights[0] + weights[1]) + (weights[2] + weights[3]), axis=1, keepdims=True)
        total = jnp.maximum(total, 1.0)
        summed = sum(dot(weights[k].astype(BF16), chunks[k][:, PAIR:]) for k in range(4))
        left = left_half((block, PAIR))
        means = jnp.where(left, summed[:block], summed[block:]) / jnp.where(
            left, total[:block], total[block:]
        )
        means = means.astype(BF16)
        lse = jnp.where(odd, peak[block:], peak[:block]) * SCALE + jnp.log(
            jnp.where(odd, total[block:], total[:block])
        )
        high = lse.astype(BF16).astype(F32)
        rest = lse - high
        middle = rest.astype(BF16).astype(F32)
        stats = jnp.where(piece == 0, high, jnp.where(piece == 1, middle, rest - middle))
        stats = jnp.where(mine, stats, 0.0 if tiling == 0 else first_stats[rows, :])
        if tiling == 0:
            stat_out[rows, :] = stats
        for d in range(block // 64):
            dest = b * (block // 64) + d
            for g in range(4):
                part = means[d * 64 + g * 16 : d * 64 + (g + 1) * 16, :]
                if tiling == 0:
                    out[dest, :, g * PAIR : (g + 1) * PAIR] = part
                else:
                    out[dest, :, 512 + g * PAIR : 512 + (g + 1) * PAIR] = part
            if tiling == 1:
                out[dest, :, :512] = first[dest]
                keep = stats[d * 64 : d * 64 + 16]
                for g in range(1, 4):
                    keep = keep + stats[d * 64 + g * 16 : d * 64 + (g + 1) * 16]
                out[dest, :, D : D + 128] = keep.astype(BF16)


def attend(tiling, count, latents, kvs, first=()):
    if tiling == 0:
        out_shape = [
            jax.ShapeDtypeStruct((PEERS, 16, 512), BF16),
            jax.ShapeDtypeStruct((LATENTS, 128), F32),
        ]
    else:
        out_shape = [jax.ShapeDtypeStruct((PEERS, 16, D + 128), BF16)]
    return pl.pallas_call(
        functools.partial(attend_body, tiling),
        out_shape=out_shape,
        in_specs=[IN_SMEM] + [IN_VMEM] * (5 + len(first)),
        out_specs=[IN_VMEM] * len(out_shape),
        compiler_params=pltpu.CompilerParams(vmem_limit_bytes=24 * MIB),
        cost_estimate=pl.CostEstimate(
            flops=4 * LATENTS * ROWS * 4 * PAIR,
            bytes_accessed=1 * MIB,
            transcendentals=LATENTS * ROWS * 8,
        ),
        name="attend",
    )(count, latents, kvs[0], kvs[3], kvs[1], kvs[2], *first)


def merge_body(parts, out):
    stats = parts[:, :, D : D + 128].reshape(PEERS * 16, 128)
    j = lax.broadcasted_iota(jnp.int32, (128, D), 0)
    n = lax.broadcasted_iota(jnp.int32, (128, D), 1)
    head = ((n >> 7) & 3) * 4 + (n >> 9) * 2 + ((n >> 6) & 1)
    spread = jnp.where(((j & 15) == head) & (j < 48), 1.0, 0.0).astype(BF16)
    lse = dot(stats, spread).reshape(PEERS, 16, D)
    peak = jnp.max(lse, axis=0)
    num = jnp.zeros((16, D), F32)
    den = jnp.zeros((16, D), F32)
    for s in range(PEERS):
        w = jnp.exp(lse[s] - peak)
        den = den + w
        num = num + w * parts[s, :, :D].astype(F32)
    att = (num / den).astype(BF16)
    for t in range(2):
        for g in range(4):
            piece = att[:, t * 512 + g * PAIR : t * 512 + (g + 1) * PAIR]
            for d in range(PEERS):
                out[d, t * 64 + g * 16 : t * 64 + (g + 1) * 16, :] = piece


def merge(parts):
    return pl.pallas_call(
        merge_body,
        out_shape=jax.ShapeDtypeStruct((PEERS, 128, PAIR), BF16),
        in_specs=[IN_VMEM],
        out_specs=IN_VMEM,
        compiler_params=pltpu.CompilerParams(vmem_limit_bytes=16 * MIB),
        cost_estimate=pl.CostEstimate(
            flops=2 * 128 * 128 * D, bytes_accessed=1 * MIB, transcendentals=128 * D
        ),
        name="merge",
    )(parts)


def half_attention(flipped, lat, same, other, wk, wv, q, enc, lk, lv):
    rows = lax.axis_index("xh") ^ flipped
    xl = lax.axis_index("xl")
    for zh in range(4):
        where = pl.multiple_of((zh * 2 + rows) * 64, 64)
        for zl in range(2):
            for t in range(2):
                for block, low in ((same, xl), (other, 1 - xl)):
                    col = pl.multiple_of((2 * zl + low) * PAIR, PAIR) + t * 512
                    enc[zh * 64 : (zh + 1) * 64, pl.ds(col, PAIR)] = lat[
                        pl.ds(where, 64), pl.ds(col, PAIR)
                    ].astype(F32) + block[2 * zh + zl, t * 64 : (t + 1) * 64, :].astype(F32)
    encoded = enc[...]
    square = jnp.sum(encoded * encoded, axis=1, keepdims=True)
    normed = (encoded * lax.rsqrt(square * (1.0 / D) + 1e-06)).astype(BF16)
    lk[...] = dot(normed, wk[...]).astype(BF16)
    lv[...] = dot(normed, wv[...]).astype(BF16)
    left = left_half((ROWS, PAIR))
    for p in range(HEADS // 2):
        cols = slice(p * PAIR, (p + 1) * PAIR)
        scores = dot_t(both_heads(q[:, cols]), lk[:, cols])
        peak = jnp.max(scores, axis=1, keepdims=True)
        weights = jnp.exp2((scores - peak) * EXP2_SCALE)
        total = jnp.sum(weights, axis=1, keepdims=True)
        summed = dot(weights.astype(BF16), lv[:, cols])
        yield (
            cols,
            jnp.where(left, summed[:ROWS], summed[ROWS:]),
            jnp.where(left, peak[:ROWS], peak[ROWS:]),
            jnp.where(left, total[:ROWS], total[ROWS:]),
        )


def near_body(lat, same, other, wk, wv, q, summed_out, peak_out, total_out, enc, lk, lv):
    for cols, summed, peak, total in half_attention(0, lat, same, other, wk, wv, q, enc, lk, lv):
        summed_out[:, cols] = summed
        peak_out[:, cols] = peak
        total_out[:, cols] = total


def far_body(lat, same, other, wk, wv, q, summed_in, peak_in, total_in, tok, out, enc, lk, lv):
    for cols, summed, peak, total in half_attention(1, lat, same, other, wk, wv, q, enc, lk, lv):
        top = jnp.maximum(peak, peak_in[:, cols])
        here = jnp.exp2((peak - top) * EXP2_SCALE)
        there = jnp.exp2((peak_in[:, cols] - top) * EXP2_SCALE)
        num = summed * here + summed_in[:, cols] * there
        den = total * here + total_in[:, cols] * there
        out[:, cols] = (tok[:, cols].astype(F32) + num / den).astype(BF16)


DECODE_SCRATCH = [
    pltpu.VMEM((LATENTS // 2, D), F32),
    pltpu.VMEM((LATENTS // 2, D), BF16),
    pltpu.VMEM((LATENTS // 2, D), BF16),
]
DECODE_COST = pl.CostEstimate(
    flops=2 * LATENTS * D * D + 2 * ROWS * LATENTS * D,
    bytes_accessed=8 * MIB,
    transcendentals=ROWS * LATENTS * HEADS // 2,
)


def decode_near(latents, same, other, wk, wv, queries):
    return pl.pallas_call(
        near_body,
        out_shape=[jax.ShapeDtypeStruct((ROWS, D), F32)] * 3,
        in_specs=[IN_VMEM] * 6,
        out_specs=[IN_VMEM] * 3,
        scratch_shapes=DECODE_SCRATCH,
        compiler_params=pltpu.CompilerParams(vmem_limit_bytes=24 * MIB),
        cost_estimate=DECODE_COST,
        name="decode_near",
    )(latents, same, other, wk, wv, queries)


def decode_far(latents, same, other, wk, wv, queries, near, tokens):
    return pl.pallas_call(
        far_body,
        out_shape=jax.ShapeDtypeStruct((ROWS, D), BF16),
        in_specs=[IN_VMEM] * 10,
        out_specs=IN_VMEM,
        scratch_shapes=DECODE_SCRATCH,
        compiler_params=pltpu.CompilerParams(vmem_limit_bytes=24 * MIB),
        cost_estimate=DECODE_COST,
        name="decode_far",
    )(latents, same, other, wk, wv, queries, *near, tokens)


def send_x(value, flip):
    pairs = [(z * NX + x, z * NX + (x ^ flip)) for z in range(NZ) for x in range(NX)]
    return lax.ppermute(value, AXES, pairs)


def per_device(
    tokens,
    valid_count,
    latents,
    key_weight,
    value_weight,
    query_weight,
    latent_key_weight,
    latent_value_weight,
):
    kv = project_kv(tokens, key_weight, value_weight)
    kvs = ([kv[0]] + [None] * 3, [kv[4]] + [None] * 3)
    for t in range(2):
        for k in (3, 1, 2):
            kvs[t][k] = send(kv[4 * t + k], k, t)
    first = attend(0, valid_count, latents, kvs[0])
    (partial,) = attend(1, valid_count, latents, kvs[1], first)
    parts = lax.all_to_all(partial, ("zh", "xh"), 0, 0, tiled=True)
    merged = merge(parts)
    rows = lax.all_to_all(merged, ("zh", "zl"), 0, 0, tiled=True)
    queries = project_queries(tokens, query_weight, rows)
    blocks = [rows] + [send_x(rows, flip) for flip in (1, 2, 3)]
    near = decode_near(
        latents, blocks[0], blocks[1], latent_key_weight, latent_value_weight, queries
    )
    return decode_far(
        latents, blocks[2], blocks[3], latent_key_weight, latent_value_weight, queries, near, tokens
    )


def solution(mesh):
    split = Mesh(mesh.devices.reshape(NZ // 2, 2, NX // 2, 2, -1), (*AXES, "reg"))
    spread = P(("reg", *AXES), None)
    placed = (spread, P("reg"), P(), P(), P(), P(), P(), P())
    return jax.shard_map(
        per_device, mesh=split, in_specs=placed, out_specs=spread, check_vma=False
    )
```

```python
import functools
import math

import jax
import jax.numpy as jnp
from jax import lax
from jax.experimental import pallas as pl
from jax.experimental.pallas import tpu as pltpu
from jax.sharding import PartitionSpec as P

D = 1024
HEADS = 16
LATENTS = 512
ROWS = 256
NX = 4
NZ = 8
PEERS = 8
PAIR = 128
GROUP = 256
SCALE = 0.125
EXP2_SCALE = SCALE * math.log2(math.e)
MIB = 1024 * 1024
KV_LIMIT = 16384


F32 = jnp.float32
BF16 = jnp.bfloat16
IN_VMEM = pl.BlockSpec(memory_space=pltpu.VMEM)
IN_HBM = pl.BlockSpec(memory_space=pltpu.HBM)
IN_SMEM = pl.BlockSpec(memory_space=pltpu.SMEM)


def dot(a, b):
    return jnp.dot(a, b, preferred_element_type=F32)


def dot_t(a, b):
    return lax.dot_general(a, b, (((1,), (1,)), ((), ())), preferred_element_type=F32)


def left_half(shape):
    return lax.broadcasted_iota(jnp.int32, shape, 1) < 64


def both_heads(pair):
    left = left_half(pair.shape)
    zero = jnp.zeros_like(pair)
    return jnp.concatenate([jnp.where(left, pair, zero), jnp.where(left, zero, pair)], axis=0)


def place():
    tok = lax.axis_index("tok")
    return tok // NX, lax.rem(tok, NX)


def send(value, target):
    pairs = []
    for z in range(NZ):
        for x in range(NX):
            tz, tx = target(z, x)
            pairs.append((z * NX + x, (tz % NZ) * NX + tx % NX))
    return lax.ppermute(value, "tok", pairs)


def colour_groups(colour):
    groups = [[], [], [], []]
    for z in range(NZ):
        for x in range(NX):
            groups[colour(z, x) % 4].append(z * NX + x)
    return groups


def exchange(value, colour):
    return lax.all_to_all(
        value, "tok", 0, 0, tiled=True, axis_index_groups=colour_groups(colour)
    )


def head_colour(z, x):
    return x + 2 * z


def gather_colour(z, x):
    return 2 * x + z


def kv_body(tok_hbm, wk_hbm, wv_hbm, *refs):
    outs, (tok, wk, wv, acc, keys, values, tok_sem, w_sem) = refs[:4], refs[4:]
    half = D // 2
    tok_copy = pltpu.make_async_copy(tok_hbm, tok, tok_sem)
    copies = []
    for n in range(2):
        rows = pl.ds(n * half, half)
        for j, (hbm, vmem) in enumerate(((wk_hbm, wk), (wv_hbm, wv))):
            copies.append(pltpu.make_async_copy(hbm.at[rows], vmem.at[rows], w_sem.at[n, j]))
    tok_copy.start()
    for c in copies:
        c.start()
    tok_copy.wait()
    for j, w in enumerate((wk, wv)):
        copies[j].wait()
        acc[j] = dot(tok[:, :half], w[:half])
    for j, (w, result) in enumerate(((wk, keys), (wv, values))):
        copies[2 + j].wait()
        result[...] = (acc[j] + dot(tok[:, half:], w[half:])).astype(BF16)
    z, x = place()
    for k in range(4):
        start = pl.multiple_of(((head_colour(z, x) + k) & 3) * GROUP, GROUP)
        outs[k][:, :GROUP] = keys[:, pl.ds(start, GROUP)]
        outs[k][:, GROUP:] = values[:, pl.ds(start, GROUP)]


def project_kv(tokens, key_weight, value_weight):
    return pl.pallas_call(
        kv_body,
        out_shape=[jax.ShapeDtypeStruct((ROWS, 2 * GROUP), BF16)] * 4,
        in_specs=[IN_HBM] * 3,
        out_specs=[IN_VMEM] * 4,
        scratch_shapes=[
            pltpu.VMEM((ROWS, D), BF16),
            pltpu.VMEM((D, D), BF16),
            pltpu.VMEM((D, D), BF16),
            pltpu.VMEM((2, ROWS, D), F32),
            pltpu.VMEM((ROWS, D), BF16),
            pltpu.VMEM((ROWS, D), BF16),
            pltpu.SemaphoreType.DMA(()),
            pltpu.SemaphoreType.DMA((2, 2)),
        ],
        compiler_params=pltpu.CompilerParams(vmem_limit_bytes=KV_LIMIT * 1024),
        cost_estimate=pl.CostEstimate(
            flops=4 * ROWS * D * D, bytes_accessed=6 * MIB, transcendentals=0
        ),
        name="kv_proj",
    )(*[pltpu.with_memory_space_constraint(a, pltpu.HBM) for a in (tokens, key_weight, value_weight)])


def query_body(tok, wq, q):
    q[...] = dot(tok[...], wq[...]).astype(BF16)


def project_queries(tokens, query_weight):
    return pl.pallas_call(
        query_body,
        out_shape=jax.ShapeDtypeStruct((ROWS, D), BF16),
        in_specs=[IN_VMEM] * 2,
        out_specs=IN_VMEM,
        compiler_params=pltpu.CompilerParams(vmem_limit_bytes=8 * MIB),
        cost_estimate=pl.CostEstimate(
            flops=2 * ROWS * D * D, bytes_accessed=3 * MIB, transcendentals=0
        ),
        name="q_proj",
    )(tokens, query_weight)


def attend_body(final, count, lat, near_kv, far_kv, *refs):
    if final:
        summed_in, peak_in, total_in, out = refs
    else:
        summed_out, peak_out, total_out = refs
    z, x = place()
    sources = ((z, x + 1), (z ^ 1, x)) if final else ((z, x), (z, x - 1))
    chunks = (near_kv, far_kv)
    lane = lax.broadcasted_iota(jnp.int32, (1, ROWS), 1)
    valid = [(sz * NX + (sx & 3)) * ROWS + lane < count[0] for sz, sx in sources]
    start = pl.multiple_of((head_colour(z, x) & 3) * GROUP, GROUP)
    block = 256
    left = left_half((block, PAIR))
    head_lane = lax.broadcasted_iota(jnp.int32, (block, 128), 1) & 3
    stat_lane = lax.broadcasted_iota(jnp.int32, (block, 128), 1)
    stat_row = lax.broadcasted_iota(jnp.int32, (block, 128), 0)
    piece = stat_lane >> 4
    mine = (((stat_lane >> 2) & 3) == ((stat_row >> 4) & 3)) & (piece < 3)
    for b in range(LATENTS // block):
        rows = slice(b * block, (b + 1) * block)
        peaks, totals, means = [], [], []
        for p in range(2):
            query = both_heads(lat[rows, pl.ds(start + p * PAIR, PAIR)])
            key_cols = slice(p * PAIR, (p + 1) * PAIR)
            value_cols = slice(GROUP + p * PAIR, GROUP + (p + 1) * PAIR)
            scores = [
                jnp.where(valid[c], dot_t(query, chunks[c][:, key_cols]), -1e30) for c in range(2)
            ]
            peak = jnp.max(jnp.maximum(scores[0], scores[1]), axis=1, keepdims=True)
            if final:
                before = jnp.concatenate(
                    [peak_in[rows, 2 * p : 2 * p + 1], peak_in[rows, 2 * p + 1 : 2 * p + 2]], axis=0
                )
                peak = jnp.maximum(peak, before)
                fade = jnp.exp2((before - peak) * EXP2_SCALE)
            else:
                peak = jnp.maximum(peak, -1e29)
            weights = [jnp.exp2((s - peak) * EXP2_SCALE) for s in scores]
            total = jnp.sum(weights[0] + weights[1], axis=1, keepdims=True)
            summed = dot(weights[0].astype(BF16), chunks[0][:, value_cols]) + dot(
                weights[1].astype(BF16), chunks[1][:, value_cols]
            )
            summed = jnp.where(left, summed[:block], summed[block:])
            if final:
                total = total + fade * jnp.concatenate(
                    [total_in[rows, 2 * p : 2 * p + 1], total_in[rows, 2 * p + 1 : 2 * p + 2]], axis=0
                )
                total = jnp.maximum(total, 1.0)
                summed = summed + summed_in[rows, key_cols] * jnp.where(
                    left, fade[:block], fade[block:]
                )
                means.append((summed / jnp.where(left, total[:block], total[block:])).astype(BF16))
            else:
                summed_out[rows, key_cols] = summed
            peaks += [peak[:block], peak[block:]]
            totals += [total[:block], total[block:]]

        def spread(parts):
            low = jnp.where(head_lane == 0, parts[0], parts[1])
            return jnp.where(head_lane < 2, low, jnp.where(head_lane == 2, parts[2], parts[3]))

        if not final:
            peak_out[rows, :] = spread(peaks)
            total_out[rows, :] = spread(totals)
            continue
        lse = spread(peaks) * SCALE + jnp.log(spread(totals))
        high = lse.astype(BF16).astype(F32)
        rest = lse - high
        middle = rest.astype(BF16).astype(F32)
        stats = jnp.where(piece == 0, high, jnp.where(piece == 1, middle, rest - middle))
        stats = jnp.where(mine, stats, 0.0)
        for d in range(block // 64):
            dest = b * (block // 64) + d
            keep = stats[d * 64 : d * 64 + 16]
            for g in range(4):
                r = slice(d * 64 + g * 16, d * 64 + (g + 1) * 16)
                for p in range(2):
                    first = g * GROUP + p * PAIR
                    out[dest, :, first : first + PAIR] = means[p][r, :]
                if g:
                    keep = keep + stats[r]
            out[dest, :, D : D + 128] = keep.astype(BF16)


def attend(final, count, latents, kvs, state=()):
    if final:
        out_shape = [jax.ShapeDtypeStruct((PEERS, 16, D + 128), BF16)]
    else:
        out_shape = [
            jax.ShapeDtypeStruct((LATENTS, GROUP), F32),
            jax.ShapeDtypeStruct((LATENTS, 128), F32),
            jax.ShapeDtypeStruct((LATENTS, 128), F32),
        ]
    return pl.pallas_call(
        functools.partial(attend_body, final),
        out_shape=out_shape,
        in_specs=[IN_SMEM] + [IN_VMEM] * (3 + len(state)),
        out_specs=[IN_VMEM] * len(out_shape),
        compiler_params=pltpu.CompilerParams(vmem_limit_bytes=24 * MIB),
        cost_estimate=pl.CostEstimate(
            flops=4 * LATENTS * ROWS * 2 * GROUP,
            bytes_accessed=1 * MIB,
            transcendentals=LATENTS * ROWS * 8,
        ),
        name="attend",
    )(count, latents, *kvs, *state)


def merge_body(parts, out):
    stats = parts[:, :, D : D + 128].reshape(PEERS * 16, 128)
    j = lax.broadcasted_iota(jnp.int32, (128, D), 0)
    n = lax.broadcasted_iota(jnp.int32, (128, D), 1)
    spread = jnp.where(((j & 15) == (n >> 6)) & (j < 48), 1.0, 0.0).astype(BF16)
    lse = dot(stats, spread).reshape(PEERS, 16, D)
    peak = jnp.max(lse, axis=0)
    num = jnp.zeros((16, D), F32)
    den = jnp.zeros((16, D), F32)
    for s in range(PEERS):
        w = jnp.exp(lse[s] - peak)
        den = den + w
        num = num + w * parts[s, :, :D].astype(F32)
    att = (num / den).astype(BF16)
    for g in range(4):
        for d in range(PEERS):
            out[d, g * 16 : (g + 1) * 16, :] = att[:, g * GROUP : (g + 1) * GROUP]


def merge(parts):
    return pl.pallas_call(
        merge_body,
        out_shape=jax.ShapeDtypeStruct((PEERS, 64, GROUP), BF16),
        in_specs=[IN_VMEM],
        out_specs=IN_VMEM,
        compiler_params=pltpu.CompilerParams(vmem_limit_bytes=16 * MIB),
        cost_estimate=pl.CostEstimate(
            flops=2 * 128 * 128 * D, bytes_accessed=1 * MIB, transcendentals=128 * D
        ),
        name="merge",
    )(parts)


def half_attention(blocks, lat, wk, wv, q, enc, lk, lv):
    for colour, block in blocks:
        for i in range(PEERS):
            z = (i >> 1) * 2 + (colour & 1)
            x = (((colour - z) >> 1) & 1) + 2 * (i & 1)
            row = pl.multiple_of(z * 64, 64)
            col = pl.multiple_of((head_colour(z, x) & 3) * GROUP, GROUP)
            enc[(i >> 1) * 64 : (i >> 1) * 64 + 64, pl.ds(col, GROUP)] = lat[
                pl.ds(row, 64), pl.ds(col, GROUP)
            ].astype(F32) + block[i].astype(F32)
    encoded = enc[...]
    square = jnp.sum(encoded * encoded, axis=1, keepdims=True)
    normed = (encoded * lax.rsqrt(square * (1.0 / D) + 1e-06)).astype(BF16)
    lk[...] = dot(normed, wk[...]).astype(BF16)
    lv[...] = dot(normed, wv[...]).astype(BF16)
    left = left_half((ROWS, PAIR))
    for p in range(HEADS // 2):
        cols = slice(p * PAIR, (p + 1) * PAIR)
        scores = dot_t(both_heads(q[:, cols]), lk[:, cols])
        peak = jnp.max(scores, axis=1, keepdims=True)
        weights = jnp.exp2((scores - peak) * EXP2_SCALE)
        total = jnp.sum(weights, axis=1, keepdims=True)
        summed = dot(weights.astype(BF16), lv[:, cols])
        yield (
            cols,
            jnp.where(left, summed[:ROWS], summed[ROWS:]),
            jnp.where(left, peak[:ROWS], peak[ROWS:]),
            jnp.where(left, total[:ROWS], total[ROWS:]),
        )


def near_body(lat, same, other, wk, wv, q, summed_out, peak_out, total_out, enc, lk, lv):
    z, x = place()
    mine = gather_colour(z, x)
    blocks = ((mine & 3, same), ((mine + 2) & 3, other))
    for cols, summed, peak, total in half_attention(blocks, lat, wk, wv, q, enc, lk, lv):
        summed_out[:, cols] = summed
        peak_out[:, cols] = peak
        total_out[:, cols] = total


def far_body(lat, below, above, wk, wv, q, summed_in, peak_in, total_in, tok, out, enc, lk, lv):
    z, x = place()
    mine = gather_colour(z, x)
    blocks = (((mine - 1) & 3, below), ((mine + 1) & 3, above))
    for cols, summed, peak, total in half_attention(blocks, lat, wk, wv, q, enc, lk, lv):
        top = jnp.maximum(peak, peak_in[:, cols])
        here = jnp.exp2((peak - top) * EXP2_SCALE)
        there = jnp.exp2((peak_in[:, cols] - top) * EXP2_SCALE)
        num = summed * here + summed_in[:, cols] * there
        den = total * here + total_in[:, cols] * there
        out[:, cols] = (tok[:, cols].astype(F32) + num / den).astype(BF16)


DECODE_SCRATCH = [
    pltpu.VMEM((LATENTS // 2, D), F32),
    pltpu.VMEM((LATENTS // 2, D), BF16),
    pltpu.VMEM((LATENTS // 2, D), BF16),
]
DECODE_COST = pl.CostEstimate(
    flops=2 * LATENTS * D * D + 2 * ROWS * LATENTS * D,
    bytes_accessed=8 * MIB,
    transcendentals=ROWS * LATENTS * HEADS // 2,
)


def decode_near(latents, same, other, wk, wv, queries):
    return pl.pallas_call(
        near_body,
        out_shape=[jax.ShapeDtypeStruct((ROWS, D), F32)] * 3,
        in_specs=[IN_VMEM] * 6,
        out_specs=[IN_VMEM] * 3,
        scratch_shapes=DECODE_SCRATCH,
        compiler_params=pltpu.CompilerParams(vmem_limit_bytes=24 * MIB),
        cost_estimate=DECODE_COST,
        name="decode_near",
    )(latents, same, other, wk, wv, queries)


def decode_far(latents, below, above, wk, wv, queries, near, tokens):
    return pl.pallas_call(
        far_body,
        out_shape=jax.ShapeDtypeStruct((ROWS, D), BF16),
        in_specs=[IN_VMEM] * 10,
        out_specs=IN_VMEM,
        scratch_shapes=DECODE_SCRATCH,
        compiler_params=pltpu.CompilerParams(vmem_limit_bytes=24 * MIB),
        cost_estimate=DECODE_COST,
        name="decode_far",
    )(latents, below, above, wk, wv, queries, *near, tokens)


def per_device(
    tokens,
    valid_count,
    latents,
    key_weight,
    value_weight,
    query_weight,
    latent_key_weight,
    latent_value_weight,
):
    own, up, across, down = project_kv(tokens, key_weight, value_weight)
    from_below = send(up, lambda z, x: (z, x + 1))
    from_above = send(down, lambda z, x: (z, x - 1))
    from_across = send(across, lambda z, x: (z ^ 1, x))
    queries = project_queries(tokens, query_weight)
    state = attend(False, valid_count, latents, (own, from_below))
    (partial,) = attend(True, valid_count, latents, (from_above, from_across), state)
    merged = merge(exchange(partial, head_colour))
    rows = exchange(merged, gather_colour)
    beside = send(rows, lambda z, x: (z, x ^ 1))
    below = send(rows, lambda z, x: (z + 1, x))
    above = send(rows, lambda z, x: (z - 1, x))
    near = decode_near(latents, rows, beside, latent_key_weight, latent_value_weight, queries)
    return decode_far(
        latents, below, above, latent_key_weight, latent_value_weight, queries, near, tokens
    )


def solution(mesh):
    spread = P(("reg", "tok"), None)
    placed = (spread, P("reg"), P(), P(), P(), P(), P(), P())
    return jax.shard_map(
        per_device, mesh=mesh, in_specs=placed, out_specs=spread, check_vma=False
    )
```

```python
import functools
import math

import jax
import jax.numpy as jnp
from jax import lax
from jax.experimental import pallas as pl
from jax.experimental.pallas import tpu as pltpu
from jax.sharding import PartitionSpec as P

D = 1024
HEADS = 16
LATENTS = 512
ROWS = 256
NX = 4
NZ = 8
PEERS = 8
PAIR = 128
GROUP = 256
SCALE = 0.125
EXP2_SCALE = SCALE * math.log2(math.e)
MIB = 1024 * 1024
KV_LIMIT = 16384


F32 = jnp.float32
BF16 = jnp.bfloat16
IN_VMEM = pl.BlockSpec(memory_space=pltpu.VMEM)
IN_HBM = pl.BlockSpec(memory_space=pltpu.HBM)
IN_SMEM = pl.BlockSpec(memory_space=pltpu.SMEM)


def dot(a, b):
    return jnp.dot(a, b, preferred_element_type=F32)


def dot_t(a, b):
    return lax.dot_general(a, b, (((1,), (1,)), ((), ())), preferred_element_type=F32)


def left_half(shape):
    return lax.broadcasted_iota(jnp.int32, shape, 1) < 64


def both_heads(pair):
    left = left_half(pair.shape)
    zero = jnp.zeros_like(pair)
    return jnp.concatenate([jnp.where(left, pair, zero), jnp.where(left, zero, pair)], axis=0)


def place():
    tok = lax.axis_index("tok")
    return tok // NX, lax.rem(tok, NX)


def send(value, target):
    pairs = []
    for z in range(NZ):
        for x in range(NX):
            tz, tx = target(z, x)
            pairs.append((z * NX + x, (tz % NZ) * NX + tx % NX))
    return lax.ppermute(value, "tok", pairs)


def colour_groups(colour):
    groups = [[], [], [], []]
    for z in range(NZ):
        for x in range(NX):
            groups[colour(z, x) % 4].append(z * NX + x)
    return groups


def exchange(value, colour):
    return lax.all_to_all(
        value, "tok", 0, 0, tiled=True, axis_index_groups=colour_groups(colour)
    )


def head_colour(z, x):
    return x + 2 * z


def gather_colour(z, x):
    return 2 * x + z


def kv_body(tok_hbm, wk_hbm, wv_hbm, *refs):
    outs, (tok, wk, wv, acc, keys, values, tok_sem, w_sem) = refs[:4], refs[4:]
    half = D // 2
    tok_copy = pltpu.make_async_copy(tok_hbm, tok, tok_sem)
    copies = []
    for n in range(2):
        rows = pl.ds(n * half, half)
        for j, (hbm, vmem) in enumerate(((wk_hbm, wk), (wv_hbm, wv))):
            copies.append(pltpu.make_async_copy(hbm.at[rows], vmem.at[rows], w_sem.at[n, j]))
    tok_copy.start()
    for c in copies:
        c.start()
    tok_copy.wait()
    for j, w in enumerate((wk, wv)):
        copies[j].wait()
        acc[j] = dot(tok[:, :half], w[:half])
    for j, (w, result) in enumerate(((wk, keys), (wv, values))):
        copies[2 + j].wait()
        result[...] = (acc[j] + dot(tok[:, half:], w[half:])).astype(BF16)
    z, x = place()
    for k in range(4):
        start = pl.multiple_of(((head_colour(z, x) + k) & 3) * GROUP, GROUP)
        outs[k][:, :GROUP] = keys[:, pl.ds(start, GROUP)]
        outs[k][:, GROUP:] = values[:, pl.ds(start, GROUP)]


def project_kv(tokens, key_weight, value_weight):
    return pl.pallas_call(
        kv_body,
        out_shape=[jax.ShapeDtypeStruct((ROWS, 2 * GROUP), BF16)] * 4,
        in_specs=[IN_HBM] * 3,
        out_specs=[IN_VMEM] * 4,
        scratch_shapes=[
            pltpu.VMEM((ROWS, D), BF16),
            pltpu.VMEM((D, D), BF16),
            pltpu.VMEM((D, D), BF16),
            pltpu.VMEM((2, ROWS, D), F32),
            pltpu.VMEM((ROWS, D), BF16),
            pltpu.VMEM((ROWS, D), BF16),
            pltpu.SemaphoreType.DMA(()),
            pltpu.SemaphoreType.DMA((2, 2)),
        ],
        compiler_params=pltpu.CompilerParams(vmem_limit_bytes=KV_LIMIT * 1024),
        cost_estimate=pl.CostEstimate(
            flops=4 * ROWS * D * D, bytes_accessed=6 * MIB, transcendentals=0
        ),
        name="kv_proj",
    )(*[pltpu.with_memory_space_constraint(a, pltpu.HBM) for a in (tokens, key_weight, value_weight)])


def query_body(tok, wq, q):
    q[...] = dot(tok[...], wq[...]).astype(BF16)


def project_queries(tokens, query_weight):
    return pl.pallas_call(
        query_body,
        out_shape=jax.ShapeDtypeStruct((ROWS, D), BF16),
        in_specs=[IN_VMEM] * 2,
        out_specs=IN_VMEM,
        compiler_params=pltpu.CompilerParams(vmem_limit_bytes=8 * MIB),
        cost_estimate=pl.CostEstimate(
            flops=2 * ROWS * D * D, bytes_accessed=3 * MIB, transcendentals=0
        ),
        name="q_proj",
    )(tokens, query_weight)


def attend_body(final, count, lat, near_kv, far_kv, *refs):
    if final:
        summed_in, peak_in, total_in, out = refs
    else:
        summed_out, peak_out, total_out = refs
    z, x = place()
    sources = ((z, x + 1), (z ^ 1, x)) if final else ((z, x), (z, x - 1))
    chunks = (near_kv, far_kv)
    lane = lax.broadcasted_iota(jnp.int32, (1, ROWS), 1)
    valid = [(sz * NX + (sx & 3)) * ROWS + lane < count[0] for sz, sx in sources]
    start = pl.multiple_of((head_colour(z, x) & 3) * GROUP, GROUP)
    block = 256
    left = left_half((block, PAIR))
    head_lane = lax.broadcasted_iota(jnp.int32, (block, 128), 1) & 3
    stat_lane = lax.broadcasted_iota(jnp.int32, (block, 128), 1)
    stat_row = lax.broadcasted_iota(jnp.int32, (block, 128), 0)
    piece = stat_lane >> 4
    mine = (((stat_lane >> 2) & 3) == ((stat_row >> 4) & 3)) & (piece < 3)
    for b in range(LATENTS // block):
        rows = slice(b * block, (b + 1) * block)
        peaks, totals, means = [], [], []
        for p in range(2):
            query = both_heads(lat[rows, pl.ds(start + p * PAIR, PAIR)])
            key_cols = slice(p * PAIR, (p + 1) * PAIR)
            value_cols = slice(GROUP + p * PAIR, GROUP + (p + 1) * PAIR)
            even = slice(2 * p * PAIR, (2 * p + 1) * PAIR)
            odd = slice((2 * p + 1) * PAIR, (2 * p + 2) * PAIR)
            scores = []
            for c in range(2):
                s = jnp.where(valid[c], dot_t(query, chunks[c][:, key_cols]), -1e30)
                scores += [s[:, :PAIR], s[:, PAIR:]]
            top = jnp.maximum(jnp.maximum(scores[0], scores[1]), jnp.maximum(scores[2], scores[3]))
            peak = jnp.broadcast_to(jnp.max(top, axis=1, keepdims=True), (2 * block, PAIR))
            if final:
                before = jnp.concatenate([peak_in[rows, even], peak_in[rows, odd]], axis=0)
                peak = jnp.maximum(peak, before)
                fade = jnp.exp2((before - peak) * EXP2_SCALE)
            else:
                peak = jnp.maximum(peak, -1e29)
            weights = [jnp.exp2((s - peak) * EXP2_SCALE) for s in scores]
            total = jnp.sum(
                (weights[0] + weights[1]) + (weights[2] + weights[3]), axis=1, keepdims=True
            )
            total = jnp.broadcast_to(total, (2 * block, PAIR))
            summed = sum(
                dot(
                    jnp.concatenate(weights[2 * c : 2 * c + 2], axis=1).astype(BF16),
                    chunks[c][:, value_cols],
                )
                for c in range(2)
            )
            summed = jnp.where(left, summed[:block], summed[block:])
            if final:
                total = total + fade * jnp.concatenate(
                    [total_in[rows, even], total_in[rows, odd]], axis=0
                )
                total = jnp.maximum(total, 1.0)
                summed = summed + summed_in[rows, key_cols] * jnp.where(
                    left, fade[:block], fade[block:]
                )
                means.append((summed / jnp.where(left, total[:block], total[block:])).astype(BF16))
            else:
                summed_out[rows, key_cols] = summed
                peak_out[rows, even] = peak[:block]
                peak_out[rows, odd] = peak[block:]
                total_out[rows, even] = total[:block]
                total_out[rows, odd] = total[block:]
            peaks += [peak[:block], peak[block:]]
            totals += [total[:block], total[block:]]

        def spread(parts):
            low = jnp.where(head_lane == 0, parts[0], parts[1])
            return jnp.where(head_lane < 2, low, jnp.where(head_lane == 2, parts[2], parts[3]))

        if not final:
            continue
        lse = spread(peaks) * SCALE + jnp.log(spread(totals))
        high = lse.astype(BF16).astype(F32)
        rest = lse - high
        middle = rest.astype(BF16).astype(F32)
        stats = jnp.where(piece == 0, high, jnp.where(piece == 1, middle, rest - middle))
        stats = jnp.where(mine, stats, 0.0)
        for d in range(block // 64):
            dest = b * (block // 64) + d
            keep = stats[d * 64 : d * 64 + 16]
            for g in range(4):
                r = slice(d * 64 + g * 16, d * 64 + (g + 1) * 16)
                for p in range(2):
                    first = g * GROUP + p * PAIR
                    out[dest, :, first : first + PAIR] = means[p][r, :]
                if g:
                    keep = keep + stats[r]
            out[dest, :, D : D + 128] = keep.astype(BF16)


def attend(final, count, latents, kvs, state=()):
    if final:
        out_shape = [jax.ShapeDtypeStruct((PEERS, 16, D + 128), BF16)]
    else:
        out_shape = [
            jax.ShapeDtypeStruct((LATENTS, GROUP), F32),
            jax.ShapeDtypeStruct((LATENTS, 4 * PAIR), F32),
            jax.ShapeDtypeStruct((LATENTS, 4 * PAIR), F32),
        ]
    return pl.pallas_call(
        functools.partial(attend_body, final),
        out_shape=out_shape,
        in_specs=[IN_SMEM] + [IN_VMEM] * (3 + len(state)),
        out_specs=[IN_VMEM] * len(out_shape),
        compiler_params=pltpu.CompilerParams(vmem_limit_bytes=24 * MIB),
        cost_estimate=pl.CostEstimate(
            flops=4 * LATENTS * ROWS * 2 * GROUP,
            bytes_accessed=1 * MIB,
            transcendentals=LATENTS * ROWS * 8,
        ),
        name="attend",
    )(count, latents, *kvs, *state)


def merge_body(parts, out):
    stats = parts[:, :, D : D + 128].reshape(PEERS * 16, 128)
    j = lax.broadcasted_iota(jnp.int32, (128, D), 0)
    n = lax.broadcasted_iota(jnp.int32, (128, D), 1)
    spread = jnp.where(((j & 15) == (n >> 6)) & (j < 48), 1.0, 0.0).astype(BF16)
    lse = dot(stats, spread).reshape(PEERS, 16, D)
    peak = jnp.max(lse, axis=0)
    num = jnp.zeros((16, D), F32)
    den = jnp.zeros((16, D), F32)
    for s in range(PEERS):
        w = jnp.exp(lse[s] - peak)
        den = den + w
        num = num + w * parts[s, :, :D].astype(F32)
    att = (num / den).astype(BF16)
    for g in range(4):
        for d in range(PEERS):
            out[d, g * 16 : (g + 1) * 16, :] = att[:, g * GROUP : (g + 1) * GROUP]


def merge(parts):
    return pl.pallas_call(
        merge_body,
        out_shape=jax.ShapeDtypeStruct((PEERS, 64, GROUP), BF16),
        in_specs=[IN_VMEM],
        out_specs=IN_VMEM,
        compiler_params=pltpu.CompilerParams(vmem_limit_bytes=16 * MIB),
        cost_estimate=pl.CostEstimate(
            flops=2 * 128 * 128 * D, bytes_accessed=1 * MIB, transcendentals=128 * D
        ),
        name="merge",
    )(parts)


def half_attention(blocks, lat, wk, wv, q, enc, lk, lv):
    for colour, block in blocks:
        for i in range(PEERS):
            z = (i >> 1) * 2 + (colour & 1)
            x = (((colour - z) >> 1) & 1) + 2 * (i & 1)
            row = pl.multiple_of(z * 64, 64)
            col = pl.multiple_of((head_colour(z, x) & 3) * GROUP, GROUP)
            enc[(i >> 1) * 64 : (i >> 1) * 64 + 64, pl.ds(col, GROUP)] = lat[
                pl.ds(row, 64), pl.ds(col, GROUP)
            ].astype(F32) + block[i].astype(F32)
    encoded = enc[...]
    square = jnp.sum(encoded * encoded, axis=1, keepdims=True)
    normed = (encoded * lax.rsqrt(square * (1.0 / D) + 1e-06)).astype(BF16)
    lk[...] = dot(normed, wk[...]).astype(BF16)
    lv[...] = dot(normed, wv[...]).astype(BF16)
    left = left_half((ROWS, PAIR))
    for p in range(HEADS // 2):
        cols = slice(p * PAIR, (p + 1) * PAIR)
        scores = dot_t(both_heads(q[:, cols]), lk[:, cols])
        peak = jnp.max(scores, axis=1, keepdims=True)
        weights = jnp.exp2((scores - peak) * EXP2_SCALE)
        total = jnp.sum(weights, axis=1, keepdims=True)
        summed = dot(weights.astype(BF16), lv[:, cols])
        yield (
            cols,
            jnp.where(left, summed[:ROWS], summed[ROWS:]),
            jnp.where(left, peak[:ROWS], peak[ROWS:]),
            jnp.where(left, total[:ROWS], total[ROWS:]),
        )


def near_body(lat, same, other, wk, wv, q, summed_out, peak_out, total_out, enc, lk, lv):
    z, x = place()
    mine = gather_colour(z, x)
    blocks = ((mine & 3, same), ((mine + 2) & 3, other))
    for cols, summed, peak, total in half_attention(blocks, lat, wk, wv, q, enc, lk, lv):
        summed_out[:, cols] = summed
        peak_out[:, cols] = peak
        total_out[:, cols] = total


def far_body(lat, below, above, wk, wv, q, summed_in, peak_in, total_in, tok, out, enc, lk, lv):
    z, x = place()
    mine = gather_colour(z, x)
    blocks = (((mine - 1) & 3, below), ((mine + 1) & 3, above))
    for cols, summed, peak, total in half_attention(blocks, lat, wk, wv, q, enc, lk, lv):
        top = jnp.maximum(peak, peak_in[:, cols])
        here = jnp.exp2((peak - top) * EXP2_SCALE)
        there = jnp.exp2((peak_in[:, cols] - top) * EXP2_SCALE)
        num = summed * here + summed_in[:, cols] * there
        den = total * here + total_in[:, cols] * there
        out[:, cols] = (tok[:, cols].astype(F32) + num / den).astype(BF16)


DECODE_SCRATCH = [
    pltpu.VMEM((LATENTS // 2, D), F32),
    pltpu.VMEM((LATENTS // 2, D), BF16),
    pltpu.VMEM((LATENTS // 2, D), BF16),
]
DECODE_COST = pl.CostEstimate(
    flops=2 * LATENTS * D * D + 2 * ROWS * LATENTS * D,
    bytes_accessed=8 * MIB,
    transcendentals=ROWS * LATENTS * HEADS // 2,
)


def decode_near(latents, same, other, wk, wv, queries):
    return pl.pallas_call(
        near_body,
        out_shape=[jax.ShapeDtypeStruct((ROWS, D), F32)] * 3,
        in_specs=[IN_VMEM] * 6,
        out_specs=[IN_VMEM] * 3,
        scratch_shapes=DECODE_SCRATCH,
        compiler_params=pltpu.CompilerParams(vmem_limit_bytes=24 * MIB),
        cost_estimate=DECODE_COST,
        name="decode_near",
    )(latents, same, other, wk, wv, queries)


def decode_far(latents, below, above, wk, wv, queries, near, tokens):
    return pl.pallas_call(
        far_body,
        out_shape=jax.ShapeDtypeStruct((ROWS, D), BF16),
        in_specs=[IN_VMEM] * 10,
        out_specs=IN_VMEM,
        scratch_shapes=DECODE_SCRATCH,
        compiler_params=pltpu.CompilerParams(vmem_limit_bytes=24 * MIB),
        cost_estimate=DECODE_COST,
        name="decode_far",
    )(latents, below, above, wk, wv, queries, *near, tokens)


def per_device(
    tokens,
    valid_count,
    latents,
    key_weight,
    value_weight,
    query_weight,
    latent_key_weight,
    latent_value_weight,
):
    own, up, across, down = project_kv(tokens, key_weight, value_weight)
    from_below = send(up, lambda z, x: (z, x + 1))
    from_above = send(down, lambda z, x: (z, x - 1))
    from_across = send(across, lambda z, x: (z ^ 1, x))
    queries = project_queries(tokens, query_weight)
    state = attend(False, valid_count, latents, (own, from_below))
    (partial,) = attend(True, valid_count, latents, (from_above, from_across), state)
    merged = merge(exchange(partial, head_colour))
    rows = exchange(merged, gather_colour)
    beside = send(rows, lambda z, x: (z, x ^ 1))
    below = send(rows, lambda z, x: (z + 1, x))
    above = send(rows, lambda z, x: (z - 1, x))
    near = decode_near(latents, rows, beside, latent_key_weight, latent_value_weight, queries)
    return decode_far(
        latents, below, above, latent_key_weight, latent_value_weight, queries, near, tokens
    )


def solution(mesh):
    spread = P(("reg", "tok"), None)
    placed = (spread, P("reg"), P(), P(), P(), P(), P(), P())
    return jax.shard_map(
        per_device, mesh=mesh, in_specs=placed, out_specs=spread, check_vma=False
    )
```

```python
import functools
import math

import jax
import jax.numpy as jnp
from jax import lax
from jax.experimental import pallas as pl
from jax.experimental.pallas import tpu as pltpu
from jax.sharding import PartitionSpec as P

D = 1024
HEADS = 16
LATENTS = 512
ROWS = 256
NX = 4
NZ = 8
PEERS = 8
PAIR = 128
GROUP = 256
SCALE = 0.125
EXP2_SCALE = SCALE * math.log2(math.e)
MIB = 1024 * 1024
KV_LIMIT = 16384


F32 = jnp.float32
BF16 = jnp.bfloat16
IN_VMEM = pl.BlockSpec(memory_space=pltpu.VMEM)
IN_HBM = pl.BlockSpec(memory_space=pltpu.HBM)
IN_SMEM = pl.BlockSpec(memory_space=pltpu.SMEM)


def dot(a, b):
    return jnp.dot(a, b, preferred_element_type=F32)


def dot_t(a, b):
    return lax.dot_general(a, b, (((1,), (1,)), ((), ())), preferred_element_type=F32)


def left_half(shape):
    return lax.broadcasted_iota(jnp.int32, shape, 1) < 64


def both_heads(pair):
    left = left_half(pair.shape)
    zero = jnp.zeros_like(pair)
    return jnp.concatenate([jnp.where(left, pair, zero), jnp.where(left, zero, pair)], axis=0)


def place():
    tok = lax.axis_index("tok")
    return tok // NX, lax.rem(tok, NX)


def send(value, target):
    pairs = []
    for z in range(NZ):
        for x in range(NX):
            tz, tx = target(z, x)
            pairs.append((z * NX + x, (tz % NZ) * NX + tx % NX))
    return lax.ppermute(value, "tok", pairs)


def colour_groups(colour):
    groups = [[], [], [], []]
    for z in range(NZ):
        for x in range(NX):
            groups[colour(z, x) % 4].append(z * NX + x)
    return groups


def exchange(value, colour):
    return lax.all_to_all(
        value, "tok", 0, 0, tiled=True, axis_index_groups=colour_groups(colour)
    )


def head_colour(z, x):
    return 2 * x + z


def gather_colour(z, x):
    return x + 2 * z


def row_block(z, x):
    return x * 2 + (z >> 2)


def kv_body(tok_hbm, wk_hbm, wv_hbm, *refs):
    outs, (tok, wk, wv, acc, keys, values, tok_sem, w_sem) = refs[:4], refs[4:]
    half = D // 2
    tok_copy = pltpu.make_async_copy(tok_hbm, tok, tok_sem)
    copies = []
    for n in range(2):
        rows = pl.ds(n * half, half)
        for j, (hbm, vmem) in enumerate(((wk_hbm, wk), (wv_hbm, wv))):
            copies.append(pltpu.make_async_copy(hbm.at[rows], vmem.at[rows], w_sem.at[n, j]))
    tok_copy.start()
    for c in copies:
        c.start()
    tok_copy.wait()
    for j, w in enumerate((wk, wv)):
        copies[j].wait()
        acc[j] = dot(tok[:, :half], w[:half])
    for j, (w, result) in enumerate(((wk, keys), (wv, values))):
        copies[2 + j].wait()
        result[...] = (acc[j] + dot(tok[:, half:], w[half:])).astype(BF16)
    z, x = place()
    for k in range(4):
        start = pl.multiple_of(((head_colour(z, x) + k) & 3) * GROUP, GROUP)
        outs[k][:, :GROUP] = keys[:, pl.ds(start, GROUP)]
        outs[k][:, GROUP:] = values[:, pl.ds(start, GROUP)]


def project_kv(tokens, key_weight, value_weight):
    return pl.pallas_call(
        kv_body,
        out_shape=[jax.ShapeDtypeStruct((ROWS, 2 * GROUP), BF16)] * 4,
        in_specs=[IN_HBM] * 3,
        out_specs=[IN_VMEM] * 4,
        scratch_shapes=[
            pltpu.VMEM((ROWS, D), BF16),
            pltpu.VMEM((D, D), BF16),
            pltpu.VMEM((D, D), BF16),
            pltpu.VMEM((2, ROWS, D), F32),
            pltpu.VMEM((ROWS, D), BF16),
            pltpu.VMEM((ROWS, D), BF16),
            pltpu.SemaphoreType.DMA(()),
            pltpu.SemaphoreType.DMA((2, 2)),
        ],
        compiler_params=pltpu.CompilerParams(vmem_limit_bytes=KV_LIMIT * 1024),
        cost_estimate=pl.CostEstimate(
            flops=4 * ROWS * D * D, bytes_accessed=6 * MIB, transcendentals=0
        ),
        name="kv_proj",
    )(*[pltpu.with_memory_space_constraint(a, pltpu.HBM) for a in (tokens, key_weight, value_weight)])


def query_body(tok, wq, q):
    q[...] = dot(tok[...], wq[...]).astype(BF16)


def project_queries(tokens, query_weight):
    return pl.pallas_call(
        query_body,
        out_shape=jax.ShapeDtypeStruct((ROWS, D), BF16),
        in_specs=[IN_VMEM] * 2,
        out_specs=IN_VMEM,
        compiler_params=pltpu.CompilerParams(vmem_limit_bytes=8 * MIB),
        cost_estimate=pl.CostEstimate(
            flops=2 * ROWS * D * D, bytes_accessed=3 * MIB, transcendentals=0
        ),
        name="q_proj",
    )(tokens, query_weight)


def attend_body(final, count, lat, near_kv, far_kv, *refs):
    if final:
        summed_in, peak_in, total_in, out = refs
    else:
        summed_out, peak_out, total_out = refs
    z, x = place()
    sources = ((z + 1, x), (z, x ^ 1)) if final else ((z, x), (z - 1, x))
    chunks = (near_kv, far_kv)
    lane = lax.broadcasted_iota(jnp.int32, (1, ROWS), 1)
    valid = [((sz & 7) * NX + sx) * ROWS + lane < count[0] for sz, sx in sources]
    start = pl.multiple_of((head_colour(z, x) & 3) * GROUP, GROUP)
    block = 256
    left = left_half((block, PAIR))
    head_lane = lax.broadcasted_iota(jnp.int32, (block, 128), 1) & 3
    stat_lane = lax.broadcasted_iota(jnp.int32, (block, 128), 1)
    stat_row = lax.broadcasted_iota(jnp.int32, (block, 128), 0)
    piece = stat_lane >> 4
    mine = (((stat_lane >> 2) & 3) == ((stat_row >> 4) & 3)) & (piece < 3)
    for b in range(LATENTS // block):
        rows = slice(b * block, (b + 1) * block)
        peaks, totals, means = [], [], []
        for p in range(2):
            query = both_heads(lat[rows, pl.ds(start + p * PAIR, PAIR)])
            key_cols = slice(p * PAIR, (p + 1) * PAIR)
            value_cols = slice(GROUP + p * PAIR, GROUP + (p + 1) * PAIR)
            even = slice(2 * p * PAIR, (2 * p + 1) * PAIR)
            odd = slice((2 * p + 1) * PAIR, (2 * p + 2) * PAIR)
            scores = []
            for c in range(2):
                s = jnp.where(valid[c], dot_t(query, chunks[c][:, key_cols]), -1e30)
                scores += [s[:, :PAIR], s[:, PAIR:]]
            top = jnp.maximum(jnp.maximum(scores[0], scores[1]), jnp.maximum(scores[2], scores[3]))
            peak = jnp.broadcast_to(jnp.max(top, axis=1, keepdims=True), (2 * block, PAIR))
            if final:
                before = jnp.concatenate([peak_in[rows, even], peak_in[rows, odd]], axis=0)
                peak = jnp.maximum(peak, before)
                fade = jnp.exp2((before - peak) * EXP2_SCALE)
            else:
                peak = jnp.maximum(peak, -1e29)
            weights = [jnp.exp2((s - peak) * EXP2_SCALE) for s in scores]
            total = jnp.sum(
                (weights[0] + weights[1]) + (weights[2] + weights[3]), axis=1, keepdims=True
            )
            total = jnp.broadcast_to(total, (2 * block, PAIR))
            summed = sum(
                dot(
                    jnp.concatenate(weights[2 * c : 2 * c + 2], axis=1).astype(BF16),
                    chunks[c][:, value_cols],
                )
                for c in range(2)
            )
            summed = jnp.where(left, summed[:block], summed[block:])
            if final:
                total = total + fade * jnp.concatenate(
                    [total_in[rows, even], total_in[rows, odd]], axis=0
                )
                total = jnp.maximum(total, 1.0)
                summed = summed + summed_in[rows, key_cols] * jnp.where(
                    left, fade[:block], fade[block:]
                )
                means.append((summed / jnp.where(left, total[:block], total[block:])).astype(BF16))
            else:
                summed_out[rows, key_cols] = summed
                peak_out[rows, even] = peak[:block]
                peak_out[rows, odd] = peak[block:]
                total_out[rows, even] = total[:block]
                total_out[rows, odd] = total[block:]
            peaks += [peak[:block], peak[block:]]
            totals += [total[:block], total[block:]]

        def spread(parts):
            low = jnp.where(head_lane == 0, parts[0], parts[1])
            return jnp.where(head_lane < 2, low, jnp.where(head_lane == 2, parts[2], parts[3]))

        if not final:
            continue
        lse = spread(peaks) * SCALE + jnp.log(spread(totals))
        high = lse.astype(BF16).astype(F32)
        rest = lse - high
        middle = rest.astype(BF16).astype(F32)
        stats = jnp.where(piece == 0, high, jnp.where(piece == 1, middle, rest - middle))
        stats = jnp.where(mine, stats, 0.0)
        for d in range(block // 64):
            owner_x, high_z = divmod(b * (block // 64) + d, 2)
            owner_z = ((head_colour(z, x) - 2 * owner_x) & 3) + 4 * high_z
            dest = (owner_z >> 1) * 2 + (owner_x >> 1)
            keep = stats[d * 64 : d * 64 + 16]
            for g in range(4):
                r = slice(d * 64 + g * 16, d * 64 + (g + 1) * 16)
                for p in range(2):
                    first = g * GROUP + p * PAIR
                    out[dest, :, first : first + PAIR] = means[p][r, :]
                if g:
                    keep = keep + stats[r]
            out[dest, :, D : D + 128] = keep.astype(BF16)


def attend(final, count, latents, kvs, state=()):
    if final:
        out_shape = [jax.ShapeDtypeStruct((PEERS, 16, D + 128), BF16)]
    else:
        out_shape = [
            jax.ShapeDtypeStruct((LATENTS, GROUP), F32),
            jax.ShapeDtypeStruct((LATENTS, 4 * PAIR), F32),
            jax.ShapeDtypeStruct((LATENTS, 4 * PAIR), F32),
        ]
    return pl.pallas_call(
        functools.partial(attend_body, final),
        out_shape=out_shape,
        in_specs=[IN_SMEM] + [IN_VMEM] * (3 + len(state)),
        out_specs=[IN_VMEM] * len(out_shape),
        compiler_params=pltpu.CompilerParams(vmem_limit_bytes=24 * MIB),
        cost_estimate=pl.CostEstimate(
            flops=4 * LATENTS * ROWS * 2 * GROUP,
            bytes_accessed=1 * MIB,
            transcendentals=LATENTS * ROWS * 8,
        ),
        name="attend",
    )(count, latents, *kvs, *state)


def merge_body(parts, out):
    stats = parts[:, :, D : D + 128].reshape(PEERS * 16, 128)
    j = lax.broadcasted_iota(jnp.int32, (128, D), 0)
    n = lax.broadcasted_iota(jnp.int32, (128, D), 1)
    spread = jnp.where(((j & 15) == (n >> 6)) & (j < 48), 1.0, 0.0).astype(BF16)
    lse = dot(stats, spread).reshape(PEERS, 16, D)
    peak = jnp.max(lse, axis=0)
    num = jnp.zeros((16, D), F32)
    den = jnp.zeros((16, D), F32)
    for s in range(PEERS):
        w = jnp.exp(lse[s] - peak)
        den = den + w
        num = num + w * parts[s, :, :D].astype(F32)
    att = (num / den).astype(BF16)
    for g in range(4):
        for d in range(PEERS):
            out[d, g * 16 : (g + 1) * 16, :] = att[:, g * GROUP : (g + 1) * GROUP]


def merge(parts):
    return pl.pallas_call(
        merge_body,
        out_shape=jax.ShapeDtypeStruct((PEERS, 64, GROUP), BF16),
        in_specs=[IN_VMEM],
        out_specs=IN_VMEM,
        compiler_params=pltpu.CompilerParams(vmem_limit_bytes=16 * MIB),
        cost_estimate=pl.CostEstimate(
            flops=2 * 128 * 128 * D, bytes_accessed=1 * MIB, transcendentals=128 * D
        ),
        name="merge",
    )(parts)


def half_attention(blocks, lat, wk, wv, q, enc, lk, lv):
    for colour, block in blocks:
        for z in range(PEERS):
            x = (colour - 2 * z) & 3
            row = pl.multiple_of(row_block(z, x) * 64, 64)
            col = pl.multiple_of((head_colour(z, x) & 3) * GROUP, GROUP)
            local = pl.multiple_of(row_block(z, x >> 1) * 64, 64)
            enc[pl.ds(local, 64), pl.ds(col, GROUP)] = lat[
                pl.ds(row, 64), pl.ds(col, GROUP)
            ].astype(F32) + block[z].astype(F32)
    encoded = enc[...]
    square = jnp.sum(encoded * encoded, axis=1, keepdims=True)
    normed = (encoded * lax.rsqrt(square * (1.0 / D) + 1e-06)).astype(BF16)
    lk[...] = dot(normed, wk[...]).astype(BF16)
    lv[...] = dot(normed, wv[...]).astype(BF16)
    left = left_half((ROWS, PAIR))
    for p in range(HEADS // 2):
        cols = slice(p * PAIR, (p + 1) * PAIR)
        scores = dot_t(both_heads(q[:, cols]), lk[:, cols])
        peak = jnp.max(scores, axis=1, keepdims=True)
        weights = jnp.exp2((scores - peak) * EXP2_SCALE)
        total = jnp.sum(weights, axis=1, keepdims=True)
        summed = dot(weights.astype(BF16), lv[:, cols])
        yield (
            cols,
            jnp.where(left, summed[:ROWS], summed[ROWS:]),
            jnp.where(left, peak[:ROWS], peak[ROWS:]),
            jnp.where(left, total[:ROWS], total[ROWS:]),
        )


def near_body(lat, same, other, wk, wv, q, summed_out, peak_out, total_out, enc, lk, lv):
    z, x = place()
    mine = gather_colour(z, x)
    blocks = ((mine & 3, same), ((mine + 2) & 3, other))
    for cols, summed, peak, total in half_attention(blocks, lat, wk, wv, q, enc, lk, lv):
        summed_out[:, cols] = summed
        peak_out[:, cols] = peak
        total_out[:, cols] = total


def far_body(lat, below, above, wk, wv, q, summed_in, peak_in, total_in, tok, out, enc, lk, lv):
    z, x = place()
    mine = gather_colour(z, x)
    blocks = (((mine - 1) & 3, below), ((mine + 1) & 3, above))
    for cols, summed, peak, total in half_attention(blocks, lat, wk, wv, q, enc, lk, lv):
        top = jnp.maximum(peak, peak_in[:, cols])
        here = jnp.exp2((peak - top) * EXP2_SCALE)
        there = jnp.exp2((peak_in[:, cols] - top) * EXP2_SCALE)
        num = summed * here + summed_in[:, cols] * there
        den = total * here + total_in[:, cols] * there
        out[:, cols] = (tok[:, cols].astype(F32) + num / den).astype(BF16)


DECODE_SCRATCH = [
    pltpu.VMEM((LATENTS // 2, D), F32),
    pltpu.VMEM((LATENTS // 2, D), BF16),
    pltpu.VMEM((LATENTS // 2, D), BF16),
]
DECODE_COST = pl.CostEstimate(
    flops=2 * LATENTS * D * D + 2 * ROWS * LATENTS * D,
    bytes_accessed=8 * MIB,
    transcendentals=ROWS * LATENTS * HEADS // 2,
)


def decode_near(latents, same, other, wk, wv, queries):
    return pl.pallas_call(
        near_body,
        out_shape=[jax.ShapeDtypeStruct((ROWS, D), F32)] * 3,
        in_specs=[IN_VMEM] * 6,
        out_specs=[IN_VMEM] * 3,
        scratch_shapes=DECODE_SCRATCH,
        compiler_params=pltpu.CompilerParams(vmem_limit_bytes=24 * MIB),
        cost_estimate=DECODE_COST,
        name="decode_near",
    )(latents, same, other, wk, wv, queries)


def decode_far(latents, below, above, wk, wv, queries, near, tokens):
    return pl.pallas_call(
        far_body,
        out_shape=jax.ShapeDtypeStruct((ROWS, D), BF16),
        in_specs=[IN_VMEM] * 10,
        out_specs=IN_VMEM,
        scratch_shapes=DECODE_SCRATCH,
        compiler_params=pltpu.CompilerParams(vmem_limit_bytes=24 * MIB),
        cost_estimate=DECODE_COST,
        name="decode_far",
    )(latents, below, above, wk, wv, queries, *near, tokens)


def per_device(
    tokens,
    valid_count,
    latents,
    key_weight,
    value_weight,
    query_weight,
    latent_key_weight,
    latent_value_weight,
):
    own, up, across, down = project_kv(tokens, key_weight, value_weight)
    from_below = send(up, lambda z, x: (z + 1, x))
    from_above = send(down, lambda z, x: (z - 1, x))
    from_across = send(across, lambda z, x: (z, x ^ 1))
    queries = project_queries(tokens, query_weight)
    state = attend(False, valid_count, latents, (own, from_below))
    (partial,) = attend(True, valid_count, latents, (from_above, from_across), state)
    merged = merge(exchange(partial, head_colour))
    rows = exchange(merged, gather_colour)
    beside = send(rows, lambda z, x: (z ^ 1, x))
    below = send(rows, lambda z, x: (z, x + 1))
    above = send(rows, lambda z, x: (z, x - 1))
    near = decode_near(latents, rows, beside, latent_key_weight, latent_value_weight, queries)
    return decode_far(
        latents, below, above, latent_key_weight, latent_value_weight, queries, near, tokens
    )


def solution(mesh):
    spread = P(("reg", "tok"), None)
    placed = (spread, P("reg"), P(), P(), P(), P(), P(), P())
    return jax.shard_map(
        per_device, mesh=mesh, in_specs=placed, out_specs=spread, check_vma=False
    )
```

```python
import functools
import math

import jax
import jax.numpy as jnp
from jax import lax
from jax.experimental import pallas as pl
from jax.experimental.pallas import tpu as pltpu
from jax.sharding import PartitionSpec as P

D = 1024
HEADS = 16
LATENTS = 512
ROWS = 256
NX = 4
NZ = 8
PEERS = 8
PAIR = 128
GROUP = 256
SCALE = 0.125
EXP2_SCALE = SCALE * math.log2(math.e)
MIB = 1024 * 1024
KV_LIMIT = 16384


F32 = jnp.float32
BF16 = jnp.bfloat16
IN_VMEM = pl.BlockSpec(memory_space=pltpu.VMEM)
IN_HBM = pl.BlockSpec(memory_space=pltpu.HBM)
IN_SMEM = pl.BlockSpec(memory_space=pltpu.SMEM)


def dot(a, b):
    return jnp.dot(a, b, preferred_element_type=F32)


def dot_t(a, b):
    return lax.dot_general(a, b, (((1,), (1,)), ((), ())), preferred_element_type=F32)


def left_half(shape):
    return lax.broadcasted_iota(jnp.int32, shape, 1) < 64


def both_heads(pair):
    left = left_half(pair.shape)
    zero = jnp.zeros_like(pair)
    return jnp.concatenate([jnp.where(left, pair, zero), jnp.where(left, zero, pair)], axis=0)


def place():
    tok = lax.axis_index("tok")
    return tok // NX, lax.rem(tok, NX)


def send(value, target):
    pairs = []
    for z in range(NZ):
        for x in range(NX):
            tz, tx = target(z, x)
            pairs.append((z * NX + x, (tz % NZ) * NX + tx % NX))
    return lax.ppermute(value, "tok", pairs)


def colour_groups(colour):
    groups = [[], [], [], []]
    for z in range(NZ):
        for x in range(NX):
            groups[colour(z, x) % 4].append(z * NX + x)
    return groups


def exchange(value, colour):
    return lax.all_to_all(
        value, "tok", 0, 0, tiled=True, axis_index_groups=colour_groups(colour)
    )


def head_colour(z, x):
    return x + 2 * z


def gather_colour(z, x):
    return 2 * x + z


def kv_body(tok_hbm, wk_hbm, wv_hbm, *refs):
    outs, (tok, wk, wv, acc, keys, values, tok_sem, w_sem) = refs[:4], refs[4:]
    half = D // 2
    tok_copy = pltpu.make_async_copy(tok_hbm, tok, tok_sem)
    copies = []
    for n in range(2):
        rows = pl.ds(n * half, half)
        for j, (hbm, vmem) in enumerate(((wk_hbm, wk), (wv_hbm, wv))):
            copies.append(pltpu.make_async_copy(hbm.at[rows], vmem.at[rows], w_sem.at[n, j]))
    tok_copy.start()
    for c in copies:
        c.start()
    tok_copy.wait()
    for j, w in enumerate((wk, wv)):
        copies[j].wait()
        acc[j] = dot(tok[:, :half], w[:half])
    for j, (w, result) in enumerate(((wk, keys), (wv, values))):
        copies[2 + j].wait()
        result[...] = (acc[j] + dot(tok[:, half:], w[half:])).astype(BF16)
    z, x = place()
    for k in range(4):
        start = pl.multiple_of(((head_colour(z, x) + k) & 3) * GROUP, GROUP)
        outs[k][:, :GROUP] = keys[:, pl.ds(start, GROUP)]
        outs[k][:, GROUP:] = values[:, pl.ds(start, GROUP)]


def project_kv(tokens, key_weight, value_weight):
    return pl.pallas_call(
        kv_body,
        out_shape=[jax.ShapeDtypeStruct((ROWS, 2 * GROUP), BF16)] * 4,
        in_specs=[IN_HBM] * 3,
        out_specs=[IN_VMEM] * 4,
        scratch_shapes=[
            pltpu.VMEM((ROWS, D), BF16),
            pltpu.VMEM((D, D), BF16),
            pltpu.VMEM((D, D), BF16),
            pltpu.VMEM((2, ROWS, D), F32),
            pltpu.VMEM((ROWS, D), BF16),
            pltpu.VMEM((ROWS, D), BF16),
            pltpu.SemaphoreType.DMA(()),
            pltpu.SemaphoreType.DMA((2, 2)),
        ],
        compiler_params=pltpu.CompilerParams(vmem_limit_bytes=KV_LIMIT * 1024),
        cost_estimate=pl.CostEstimate(
            flops=4 * ROWS * D * D, bytes_accessed=6 * MIB, transcendentals=0
        ),
        name="kv_proj",
    )(*[pltpu.with_memory_space_constraint(a, pltpu.HBM) for a in (tokens, key_weight, value_weight)])


def query_body(tok, wq, q):
    q[...] = dot(tok[...], wq[...]).astype(BF16)


def project_queries(tokens, query_weight):
    return pl.pallas_call(
        query_body,
        out_shape=jax.ShapeDtypeStruct((ROWS, D), BF16),
        in_specs=[IN_VMEM] * 2,
        out_specs=IN_VMEM,
        compiler_params=pltpu.CompilerParams(vmem_limit_bytes=8 * MIB),
        cost_estimate=pl.CostEstimate(
            flops=2 * ROWS * D * D, bytes_accessed=3 * MIB, transcendentals=0
        ),
        name="q_proj",
    )(tokens, query_weight)


def attend_body(final, count, lat, near_kv, far_kv, *refs):
    if final:
        summed_in, peak_in, total_in, out = refs
    else:
        summed_out, peak_out, total_out = refs
    z, x = place()
    sources = ((z, x + 1), (z ^ 1, x)) if final else ((z, x), (z, x - 1))
    chunks = (near_kv, far_kv)
    lane = lax.broadcasted_iota(jnp.int32, (1, ROWS), 1)
    valid = [(sz * NX + (sx & 3)) * ROWS + lane < count[0] for sz, sx in sources]
    start = pl.multiple_of((head_colour(z, x) & 3) * GROUP, GROUP)
    block = 256
    left = left_half((block, PAIR))
    head_lane = lax.broadcasted_iota(jnp.int32, (block, 128), 1) & 3
    stat_lane = lax.broadcasted_iota(jnp.int32, (block, 128), 1)
    stat_row = lax.broadcasted_iota(jnp.int32, (block, 128), 0)
    piece = stat_lane >> 4
    mine = (((stat_lane >> 2) & 3) == ((stat_row >> 4) & 3)) & (piece < 3)
    for b in range(LATENTS // block):
        rows = slice(b * block, (b + 1) * block)
        peaks, totals, means = [], [], []
        for p in range(2):
            query = both_heads(lat[rows, pl.ds(start + p * PAIR, PAIR)])
            key_cols = slice(p * PAIR, (p + 1) * PAIR)
            value_cols = slice(GROUP + p * PAIR, GROUP + (p + 1) * PAIR)
            even = slice(2 * p * PAIR, (2 * p + 1) * PAIR)
            odd = slice((2 * p + 1) * PAIR, (2 * p + 2) * PAIR)
            scores = []
            for c in range(2):
                s = jnp.where(valid[c], dot_t(query, chunks[c][:, key_cols]), -1e30)
                scores += [s[:, :PAIR], s[:, PAIR:]]
            top = jnp.maximum(jnp.maximum(scores[0], scores[1]), jnp.maximum(scores[2], scores[3]))
            peak = jnp.broadcast_to(jnp.max(top, axis=1, keepdims=True), (2 * block, PAIR))
            if final:
                before = jnp.concatenate([peak_in[rows, even], peak_in[rows, odd]], axis=0)
                peak = jnp.maximum(peak, before)
                fade = jnp.exp2((before - peak) * EXP2_SCALE)
            else:
                peak = jnp.maximum(peak, -1e29)
            weights = [jnp.exp2((s - peak) * EXP2_SCALE) for s in scores]
            total = jnp.sum(
                (weights[0] + weights[1]) + (weights[2] + weights[3]), axis=1, keepdims=True
            )
            total = jnp.broadcast_to(total, (2 * block, PAIR))
            summed = sum(
                dot(
                    jnp.concatenate(weights[2 * c : 2 * c + 2], axis=1).astype(BF16),
                    chunks[c][:, value_cols],
                )
                for c in range(2)
            )
            summed = jnp.where(left, summed[:block], summed[block:])
            if final:
                total = total + fade * jnp.concatenate(
                    [total_in[rows, even], total_in[rows, odd]], axis=0
                )
                total = jnp.maximum(total, 1.0)
                summed = summed + summed_in[rows, key_cols] * jnp.where(
                    left, fade[:block], fade[block:]
                )
                means.append((summed / jnp.where(left, total[:block], total[block:])).astype(BF16))
            else:
                summed_out[rows, key_cols] = summed
                peak_out[rows, even] = peak[:block]
                peak_out[rows, odd] = peak[block:]
                total_out[rows, even] = total[:block]
                total_out[rows, odd] = total[block:]
            peaks += [peak[:block], peak[block:]]
            totals += [total[:block], total[block:]]

        def spread(parts):
            low = jnp.where(head_lane == 0, parts[0], parts[1])
            return jnp.where(head_lane < 2, low, jnp.where(head_lane == 2, parts[2], parts[3]))

        if not final:
            continue
        lse = spread(peaks) * SCALE + jnp.log(spread(totals))
        high = lse.astype(BF16).astype(F32)
        rest = lse - high
        middle = rest.astype(BF16).astype(F32)
        stats = jnp.where(piece == 0, high, jnp.where(piece == 1, middle, rest - middle))
        stats = jnp.where(mine, stats, 0.0)
        for d in range(block // 64):
            dest = b * (block // 64) + d
            keep = stats[d * 64 : d * 64 + 16]
            for g in range(4):
                r = slice(d * 64 + g * 16, d * 64 + (g + 1) * 16)
                for p in range(2):
                    first = g * GROUP + p * PAIR
                    out[dest, :, first : first + PAIR] = means[p][r, :]
                if g:
                    keep = keep + stats[r]
            out[dest, :, D : D + 128] = keep.astype(BF16)


def attend(final, count, latents, kvs, state=()):
    if final:
        out_shape = [jax.ShapeDtypeStruct((PEERS, 16, D + 128), BF16)]
    else:
        out_shape = [
            jax.ShapeDtypeStruct((LATENTS, GROUP), F32),
            jax.ShapeDtypeStruct((LATENTS, 4 * PAIR), F32),
            jax.ShapeDtypeStruct((LATENTS, 4 * PAIR), F32),
        ]
    return pl.pallas_call(
        functools.partial(attend_body, final),
        out_shape=out_shape,
        in_specs=[IN_SMEM] + [IN_VMEM] * (3 + len(state)),
        out_specs=[IN_VMEM] * len(out_shape),
        compiler_params=pltpu.CompilerParams(vmem_limit_bytes=24 * MIB),
        cost_estimate=pl.CostEstimate(
            flops=4 * LATENTS * ROWS * 2 * GROUP,
            bytes_accessed=1 * MIB,
            transcendentals=LATENTS * ROWS * 8,
        ),
        name="attend",
    )(count, latents, *kvs, *state)


def merge_body(parts, out):
    stats = parts[:, :, D : D + 128].reshape(PEERS * 16, 128)
    j = lax.broadcasted_iota(jnp.int32, (128, D), 0)
    n = lax.broadcasted_iota(jnp.int32, (128, D), 1)
    spread = jnp.where(((j & 15) == (n >> 6)) & (j < 48), 1.0, 0.0).astype(BF16)
    lse = dot(stats, spread).reshape(PEERS, 16, D)
    peak = jnp.max(lse, axis=0)
    num = jnp.zeros((16, D), F32)
    den = jnp.zeros((16, D), F32)
    for s in range(PEERS):
        w = jnp.exp(lse[s] - peak)
        den = den + w
        num = num + w * parts[s, :, :D].astype(F32)
    att = (num / den).astype(BF16)
    for g in range(4):
        for d in range(PEERS):
            out[d, g * 16 : (g + 1) * 16, :] = att[:, g * GROUP : (g + 1) * GROUP]


def merge(parts):
    return pl.pallas_call(
        merge_body,
        out_shape=jax.ShapeDtypeStruct((PEERS, 64, GROUP), BF16),
        in_specs=[IN_VMEM],
        out_specs=IN_VMEM,
        compiler_params=pltpu.CompilerParams(vmem_limit_bytes=16 * MIB),
        cost_estimate=pl.CostEstimate(
            flops=2 * 128 * 128 * D, bytes_accessed=1 * MIB, transcendentals=128 * D
        ),
        name="merge",
    )(parts)


def half_attention(blocks, lat, wk, wv, q, enc, lk, lv):
    for colour, block in blocks:
        for i in range(PEERS):
            z = (i >> 1) * 2 + (colour & 1)
            x = (((colour - z) >> 1) & 1) + 2 * (i & 1)
            row = pl.multiple_of(z * 64, 64)
            col = pl.multiple_of((head_colour(z, x) & 3) * GROUP, GROUP)
            enc[(i >> 1) * 64 : (i >> 1) * 64 + 64, pl.ds(col, GROUP)] = lat[
                pl.ds(row, 64), pl.ds(col, GROUP)
            ].astype(F32) + block[i].astype(F32)
    encoded = enc[...]
    square = jnp.sum(encoded * encoded, axis=1, keepdims=True)
    normed = (encoded * lax.rsqrt(square * (1.0 / D) + 1e-06)).astype(BF16)
    lk[...] = dot(normed, wk[...]).astype(BF16)
    lv[...] = dot(normed, wv[...]).astype(BF16)
    left = left_half((ROWS, PAIR))
    for p in range(HEADS // 2):
        cols = slice(p * PAIR, (p + 1) * PAIR)
        scores = dot_t(both_heads(q[:, cols]), lk[:, cols])
        peak = jnp.max(scores, axis=1, keepdims=True)
        weights = jnp.exp2((scores - peak) * EXP2_SCALE)
        total = jnp.sum(weights, axis=1, keepdims=True)
        summed = dot(weights.astype(BF16), lv[:, cols])
        yield (
            cols,
            jnp.where(left, summed[:ROWS], summed[ROWS:]),
            jnp.where(left, peak[:ROWS], peak[ROWS:]),
            jnp.where(left, total[:ROWS], total[ROWS:]),
        )


def near_body(lat, same, other, wk, wv, q, summed_out, peak_out, total_out, enc, lk, lv):
    z, x = place()
    mine = gather_colour(z, x)
    blocks = ((mine & 3, same), ((mine + 2) & 3, other))
    for cols, summed, peak, total in half_attention(blocks, lat, wk, wv, q, enc, lk, lv):
        summed_out[:, cols] = summed
        peak_out[:, cols] = peak
        total_out[:, cols] = total


def far_body(lat, below, above, wk, wv, q, summed_in, peak_in, total_in, tok, out, enc, lk, lv):
    z, x = place()
    mine = gather_colour(z, x)
    blocks = (((mine - 1) & 3, below), ((mine + 1) & 3, above))
    for cols, summed, peak, total in half_attention(blocks, lat, wk, wv, q, enc, lk, lv):
        top = jnp.maximum(peak, peak_in[:, cols])
        here = jnp.exp2((peak - top) * EXP2_SCALE)
        there = jnp.exp2((peak_in[:, cols] - top) * EXP2_SCALE)
        num = summed * here + summed_in[:, cols] * there
        den = total * here + total_in[:, cols] * there
        out[:, cols] = (tok[:, cols].astype(F32) + num / den).astype(BF16)


DECODE_SCRATCH = [
    pltpu.VMEM((LATENTS // 2, D), F32),
    pltpu.VMEM((LATENTS // 2, D), BF16),
    pltpu.VMEM((LATENTS // 2, D), BF16),
]
DECODE_COST = pl.CostEstimate(
    flops=2 * LATENTS * D * D + 2 * ROWS * LATENTS * D,
    bytes_accessed=8 * MIB,
    transcendentals=ROWS * LATENTS * HEADS // 2,
)


def decode_near(latents, same, other, wk, wv, queries):
    return pl.pallas_call(
        near_body,
        out_shape=[jax.ShapeDtypeStruct((ROWS, D), F32)] * 3,
        in_specs=[IN_VMEM] * 6,
        out_specs=[IN_VMEM] * 3,
        scratch_shapes=DECODE_SCRATCH,
        compiler_params=pltpu.CompilerParams(vmem_limit_bytes=24 * MIB),
        cost_estimate=DECODE_COST,
        name="decode_near",
    )(latents, same, other, wk, wv, queries)


def decode_far(latents, below, above, wk, wv, queries, near, tokens):
    return pl.pallas_call(
        far_body,
        out_shape=jax.ShapeDtypeStruct((ROWS, D), BF16),
        in_specs=[IN_VMEM] * 10,
        out_specs=IN_VMEM,
        scratch_shapes=DECODE_SCRATCH,
        compiler_params=pltpu.CompilerParams(vmem_limit_bytes=24 * MIB),
        cost_estimate=DECODE_COST,
        name="decode_far",
    )(latents, below, above, wk, wv, queries, *near, tokens)


def per_device(
    tokens,
    valid_count,
    latents,
    key_weight,
    value_weight,
    query_weight,
    latent_key_weight,
    latent_value_weight,
):
    own, up, across, down = project_kv(tokens, key_weight, value_weight)
    from_below = send(up, lambda z, x: (z, x + 1))
    from_above = send(down, lambda z, x: (z, x - 1))
    from_across = send(across, lambda z, x: (z ^ 1, x))
    queries = project_queries(tokens, query_weight)
    own, queries = lax.optimization_barrier((own, queries))
    state = attend(False, valid_count, latents, (own, from_below))
    (partial,) = attend(True, valid_count, latents, (from_above, from_across), state)
    merged = merge(exchange(partial, head_colour))
    rows = exchange(merged, gather_colour)
    beside = send(rows, lambda z, x: (z, x ^ 1))
    below = send(rows, lambda z, x: (z + 1, x))
    above = send(rows, lambda z, x: (z - 1, x))
    near = decode_near(latents, rows, beside, latent_key_weight, latent_value_weight, queries)
    return decode_far(
        latents, below, above, latent_key_weight, latent_value_weight, queries, near, tokens
    )


def solution(mesh):
    spread = P(("reg", "tok"), None)
    placed = (spread, P("reg"), P(), P(), P(), P(), P(), P())
    return jax.shard_map(
        per_device, mesh=mesh, in_specs=placed, out_specs=spread, check_vma=False
    )
```
